256 devices in a mesh: dp: 32 (over y, z), group: 8 (over x, core).
Axes of the slice: x: 4, y: 4, z: 8, core: 2. Of those that a mesh axis runs over, the one named last changes fastest.
Arguments:
- keys: int32 [131072], P(('dp', 'group')), may hold values from 0 to 1073741823
- cut: int32 [1], replicated, may hold values from 256 to 1023
- owner: int32 [131072, 1], P(('dp', 'group')), may hold values from 0 to 31; in each aligned block of 512 rows (0 to 511, 512 to 1023, ...) at most 32 rows name the same one
- tokens: int32 [131072, 2048], P(('dp', 'group')), may hold values from 0 to 128255
Outputs:
- histogram: int32 [4096], replicated
- packed_rows: int32 [262144, 2048], P(('dp', 'group'))
- packed_weights: float32 [262144], P(('dp', 'group'))
The draws below stay inside these ranges and needn't reach their ends.
Inputs may be any that keep to these rules, and one draw needn't show every extreme that they name: Among the examples of one device, at most 32 have the same owner, and some owner has exactly 32.
All inputs are finite; a program needn't handle non-finite values.
Results may differ from the reference program's by a relative error of at most 0.0003.
Values sent between devices are 32-bit elements; how exact they have to be, the bound alone decides.
A program may use at most 128 MiB of HBM per device.

```python
import math
import jax
import jax.numpy as jnp
import numpy as np

EX_DEV = 512
SEQ = 2048
BINS = 4096
BIN_WIDTH = 262144
VOCAB = 128256
EXAMPLES = 131072
MOST = 32
RECV = 1024
N_DP = 32
N_GROUP = 8


def place_ends(array, rng, smallest, top_value):
    extent = array.shape
    place = [jax.random.randint(jax.random.fold_in(rng, axis), (), 0, extent[axis]) for axis in range(len(extent))]
    array = array.at[tuple(place)].set(smallest)
    longest = extent.index(max(extent))
    place[longest] = (place[longest] + 1) % extent[longest]
    return array.at[tuple(place)].set(top_value)


def ranked_wide(rng, extent, amount, slope):
    weights = [min(1 << octave, amount + 1 - (1 << octave)) * (1 << 20) // math.isqrt((1 << octave) ** slope) + 1 for octave in range((amount + 1).bit_length()) if 1 << octave <= amount]
    scale = 1 + sum(weights) // (1 << 30)
    table = np.cumsum(np.array([max(1, weight // scale) for weight in weights]))
    ticket = jax.random.randint(jax.random.fold_in(rng, 1), extent, 0, int(table[len(weights) - 1]))
    start = jnp.left_shift(1, jnp.searchsorted(jnp.asarray(table, jnp.int32), ticket, side="right").astype(jnp.int32))
    rank = start - 1 + jax.random.randint(jax.random.fold_in(rng, 4), extent, 0, 1 << 30) % jnp.minimum(start, amount + 1 - start)
    return jax.random.permutation(jax.random.fold_in(rng, 2), amount)[rank].astype(jnp.int32)


def deal_out(rng, own, number, rows, number_of, top, limit, slope):
    ranking = jax.random.permutation(rng, number_of)
    packed, common = shares(number_of, rows * top, limit, slope, True), shares(number_of, rows * top, limit, slope, False)
    places = jnp.arange(number_of)

    def named(sizes, rotation):
        used = int((sizes > 0).sum())
        fixed = max(1, used // 4)
        moved = fixed + (places - fixed + rotation * (used - fixed)) % max(1, number_of - fixed)
        return jnp.zeros((number_of,), jnp.int32).at[ranking[jnp.where(places < fixed, places, moved)]].set(jnp.asarray(sizes, jnp.int32))

    sizes = jnp.where(number % 4 == 0, named(packed, number // 4), named(common, number - number // 4 - 1))
    mixed = jax.random.permutation(jax.random.fold_in(own, 3), number_of)
    donor, taker = mixed[0:number_of // 2 * 2:2], mixed[1:number_of // 2 * 2:2]
    margin = jnp.minimum(sizes[donor] - 1, limit - sizes[taker]) // 2
    margin = jnp.where((donor == ranking[0]) | (taker == ranking[0]) | (sizes[taker] == 0), 0, jnp.maximum(margin, 0))
    moved = jax.random.randint(jax.random.fold_in(own, 4), (number_of // 2,), 0, 1 << 20) % (margin + 1)
    sizes = sizes.at[donor].add(-moved).at[taker].add(moved)
    members = jnp.searchsorted(jnp.cumsum(sizes), jnp.arange(rows * top), side="right").astype(jnp.int32)
    table = members.reshape(top, rows).T
    table = table[jax.random.permutation(jax.random.fold_in(own, 1), rows)]
    rotation = jax.random.randint(jax.random.fold_in(own, 2), (rows, 1), 0, top)
    return jnp.take_along_axis(table, (jnp.arange(top)[None, :] + rotation) % top, axis=1)


def shares(count, total, bound, slope, full):
    weights = [(1 << 20) // math.isqrt(standing ** slope) + 1 for standing in range(1, count + 1)]
    largest = bound if full else min(bound, max(-(-total // count), total * weights[0] // sum(weights)))
    least = 1 if total - largest >= count - 1 else 0
    counts, spare = [largest] + [least] * (count - 1), total - largest - least * (count - 1)
    while spare > 0:
        free = [i for i in range(1, count) if counts[i] < largest] or [i for i in range(1, count) if counts[i] < bound]
        mass, remaining = sum([weights[i] for i in free]), spare
        for i in free:
            more = min(bound - counts[i], max(1, remaining * weights[i] // mass), spare)
            counts[i] = counts[i] + more
            spare = spare - more
    return np.array(counts)


def setup_inputs(seed: int = 0) -> dict:
    splits = jax.random.split(jax.random.key(seed), 5)
    keys = place_ends(jax.random.randint(splits[0], (EXAMPLES,), 0, BINS * BIN_WIDTH), jax.random.fold_in(splits[0], 1), 0, (BINS * BIN_WIDTH) - 1).astype(jnp.int32)
    cut = jax.random.randint(splits[1], (1,), BINS // 16, BINS // 4).astype(jnp.int32)
    owner_keys = jax.random.split(jax.random.fold_in(splits[2], 1), EXAMPLES // EX_DEV)
    owner_turns = jax.random.permutation(jax.random.fold_in(splits[2], 3), EXAMPLES // EX_DEV)
    owner = jax.vmap(lambda own, number: deal_out(jax.random.fold_in(splits[2], 2), own, number, EX_DEV, N_DP, 1, MOST, 2))(owner_keys, owner_turns).reshape((EXAMPLES, 1))
    tokens = place_ends(ranked_wide(splits[3], (EXAMPLES, SEQ), VOCAB, 2), jax.random.fold_in(splits[3], 3), 0, VOCAB - 1).astype(jnp.int32)
    return {"keys": keys, "cut": cut, "owner": owner, "tokens": tokens}


def reference(keys, cut, owner, tokens):
    bins_of = keys // BIN_WIDTH
    hist = jnp.zeros((BINS,), jnp.float32).at[bins_of].add(1.0)
    kept = bins_of >= cut[0]
    dest = owner[:, 0]
    onehot = ((dest[:, None] == jnp.arange(N_DP, dtype=jnp.int32)[None, :]) & kept[:, None]).astype(jnp.int32)
    running = jnp.cumsum(onehot, axis=0) - onehot
    rank = jnp.sum(running * onehot, axis=1)
    device = dest * N_GROUP + rank % N_GROUP
    slot = rank // N_GROUP
    count = N_DP * N_GROUP * RECV
    target = jnp.where(kept, device * RECV + slot, count).astype(jnp.int32)
    suffix = jnp.cumsum(hist[::-1])[::-1]
    total = jnp.maximum(suffix[cut[0]], 1.0)
    weight = suffix[bins_of] / total
    packed_rows = jnp.zeros((count, SEQ), jnp.int32).at[target].set(tokens, mode="drop")
    packed_weights = jnp.zeros((count,), jnp.float32).at[target].set(weight, mode="drop")
    return hist.astype(jnp.int32), packed_rows, packed_weights
```

```python
import functools

import jax
import jax.numpy as jnp
from jax import lax
from jax.experimental import pallas as pl
from jax.experimental.pallas import tpu as pltpu
from jax.sharding import Mesh
from jax.sharding import PartitionSpec as P

BINS = 4096
BIN_WIDTH = 262144
NY, NZ, NX, NC = 4, 8, 4, 2
NO = NY * NZ
NM = NX * NC
NS = NO * NM
PLANE = NY * NM
EX = 512
RECV = 1024
MESH_ID = pl.DeviceIdType.MESH
AXES = ("y", "z", "x", "c")

TIERS = (
    (208, 168, 120, 72),
    (232, 192, 136, 80),
    (256, 208, 152, 96),
    (384, 264, 256, 128),
)
PLUS, OWN, MINUS = 0, 384, 512
PACKED = 896


def me():
    return tuple(lax.axis_index(a) for a in AXES)


def signal_peers(bar, z, y, x, c):
    def ring(d, _):
        pl.semaphore_signal(bar, 1, device_id={"z": lax.rem(z + d, NZ)}, device_id_type=MESH_ID)
        return 0

    def plane(r, _):
        pl.semaphore_signal(bar, 1, device_id=in_plane(r, y, x, c), device_id_type=MESH_ID)
        return 0

    lax.fori_loop(1, NZ, ring, 0)
    lax.fori_loop(1, PLANE, plane, 0)
    pl.semaphore_wait(bar, NZ - 1 + PLANE - 1)


def in_plane(r, y, x, c):
    return {
        "y": lax.rem(y + r // NM, NY),
        "x": lax.rem(x + (r // NC) % NX, NX),
        "c": lax.rem(c + r % NC, NC),
    }


def counts_kernel(row_ref, out_ref, ring_ref, send1, send2, recv1, recv2):
    y, z, x, c = me()
    signal_peers(pltpu.get_barrier_semaphore(), z, y, x, c)

    def ring_copy(d):
        return pltpu.make_async_remote_copy(
            row_ref.at[0], ring_ref.at[z], send1, recv1,
            device_id={"z": lax.rem(z + d, NZ)}, device_id_type=MESH_ID)

    def start_ring(d, _):
        ring_copy(d).start()
        return 0

    lax.fori_loop(1, NZ, start_ring, 0)
    pltpu.make_async_copy(row_ref.at[0], ring_ref.at[z], recv1).start()
    pltpu.make_async_copy(ring_ref, ring_ref, recv1).wait()
    p = y * NM + x * NC + c

    def start_plane(r, _):
        pltpu.make_async_remote_copy(
            ring_ref, out_ref.at[p], send2, recv2,
            device_id=in_plane(r, y, x, c), device_id_type=MESH_ID).start()
        return 0

    lax.fori_loop(1, PLANE, start_plane, 0)
    out_ref[pl.ds(p, 1)] = ring_ref[...].reshape(1, NZ, 1, 128)
    pltpu.make_async_copy(out_ref.at[pl.ds(0, PLANE - 1)], out_ref.at[pl.ds(0, PLANE - 1)], recv2).wait()
    pltpu.make_async_copy(ring_ref.at[pl.ds(0, NZ - 1)], ring_ref.at[pl.ds(0, NZ - 1)], send1).wait()
    pltpu.make_async_copy(out_ref.at[pl.ds(0, PLANE - 1)], out_ref.at[pl.ds(0, PLANE - 1)], send2).wait()


def exchange_counts(row):
    return pl.pallas_call(
        counts_kernel,
        out_shape=jax.ShapeDtypeStruct((PLANE, NZ, 1, 128), jnp.int32),
        in_specs=[pl.BlockSpec(memory_space=pltpu.VMEM)],
        out_specs=pl.BlockSpec(memory_space=pltpu.VMEM),
        scratch_shapes=[
            pltpu.VMEM((NZ, 1, 128), jnp.int32),
            pltpu.SemaphoreType.DMA, pltpu.SemaphoreType.DMA, pltpu.SemaphoreType.DMA, pltpu.SemaphoreType.DMA,
        ],
        compiler_params=pltpu.CompilerParams(collective_id=0, has_side_effects=True),
        name="exchange_counts",
    )(row)


def pack_kernel(pos_ref, tok_ref, out_ref):
    def row(e, _):
        p = pos_ref[e]

        @pl.when(p >= 0)
        def _():
            start = (e // 8) * 128 + e % 8
            out_ref[pl.ds(pl.multiple_of(p * 16, 16), 16), :] = tok_ref[pl.ds(start, 16, stride=8), :]

        return 0

    lax.fori_loop(0, EX, row, 0, unroll=4)


def pack_rows(pos, tok):
    return pl.pallas_call(
        pack_kernel,
        out_shape=jax.ShapeDtypeStruct((PACKED * 16, 128), jnp.int32),
        in_specs=[pl.BlockSpec(memory_space=pltpu.SMEM), pl.BlockSpec(memory_space=pltpu.VMEM)],
        out_specs=pl.BlockSpec(memory_space=pltpu.VMEM),
        name="pack_rows",
    )(pos, tok)


def main_kernel(caps, idx_ref, pk_ref, bin_ref, hist_ref,
                rows_out, hist_out, bins_out,
                p1, m1, p2, m2, p3, m3, far, stage, hz, hp, bz,
                zsend, zrecv, psend, precv, hzsend, hzrecv, hpsend, hprecv, bzsend, bzrecv, bpsend, bprecv):
    y, z, x, c = me()
    signal_peers(pltpu.get_barrier_semaphore(), z, y, x, c)
    c1, c2, c3, c4 = caps
    up, down = lax.rem(z + 1, NZ), lax.rem(z + NZ - 1, NZ)
    plane = y * NM + x * NC + c

    def hop(src, dst, lo, hi, at_src, at_dst, sem, to):
        copy = pltpu.make_async_remote_copy(
            src.at[pl.ds(at_src + lo, hi - lo)],
            dst.at[pl.ds(at_dst + lo, hi - lo)],
            zsend.at[sem], zrecv.at[sem], device_id={"z": to}, device_id_type=MESH_ID)
        copy.start()
        return copy

    h1 = [hop(pk_ref, p1, 0, c2, PLUS, 0, 0, up), hop(pk_ref, m1, 0, c2, MINUS, 0, 1, down),
          hop(pk_ref, p1, c2, c1, PLUS, 0, 2, up), hop(pk_ref, m1, c2, c1, MINUS, 0, 3, down)]

    def ring_small(d, _):
        to = {"z": lax.rem(z + d, NZ)}
        pltpu.make_async_remote_copy(hist_ref, hz.at[z], hzsend, hzrecv, device_id=to, device_id_type=MESH_ID).start()
        pltpu.make_async_remote_copy(bin_ref, bz.at[z], bzsend, bzrecv, device_id=to, device_id_type=MESH_ID).start()
        return 0

    lax.fori_loop(1, NZ, ring_small, 0)
    hz[pl.ds(z, 1)] = hist_ref[...].reshape(1, 32, 128)
    bz[pl.ds(z, 1)] = bin_ref[...].reshape(1, 4, 128)

    def send_chunk(delta, src):
        base = delta * PLANE * 4

        def gather(i, _):
            stage[base + i] = src[idx_ref[base + i]]
            return 0

        lax.fori_loop(0, PLANE * 4, gather, 0, unroll=8)
        zs = lax.rem(z + NZ - delta, NZ)
        s = ((y * NZ + zs) * NX + x) * NC + c

        def send(r, _):
            pltpu.make_async_remote_copy(
                stage.at[pl.ds((delta * PLANE + r) * 4, 4)],
                rows_out.at[pl.ds(s * 4, 4)],
                psend, precv, device_id=in_plane(r, y, x, c), device_id_type=MESH_ID).start()
            return 0

        lax.fori_loop(1, PLANE, send, 0)
        pltpu.make_async_copy(stage.at[pl.ds(delta * PLANE * 4, 4)], rows_out.at[pl.ds(s * 4, 4)], precv).start()

    send_chunk(0, pk_ref)

    seven = hz.at[pl.ds(0, NZ - 1)]
    pltpu.make_async_copy(seven, seven, hzrecv).wait()
    seven_b = bz.at[pl.ds(0, NZ - 1)]
    pltpu.make_async_copy(seven_b, seven_b, bzrecv).wait()
    total = hz[0]
    for k in range(1, NZ):
        total = total + hz[k]
    hp[pl.ds(plane, 1)] = total.reshape(1, 32, 128)
    bins_out[pl.ds(plane, 1)] = bz[...].reshape(1, NZ, 4, 128)

    def plane_small(r, _):
        to = in_plane(r, y, x, c)
        pltpu.make_async_remote_copy(hp.at[plane], hp.at[plane], hpsend, hprecv, device_id=to, device_id_type=MESH_ID).start()
        pltpu.make_async_remote_copy(bz, bins_out.at[plane], bpsend, bprecv, device_id=to, device_id_type=MESH_ID).start()
        return 0

    lax.fori_loop(1, PLANE, plane_small, 0)
    others = hp.at[pl.ds(0, PLANE - 1)]
    pltpu.make_async_copy(others, others, hprecv).wait()
    others_b = bins_out.at[pl.ds(0, PLANE - 1)]
    pltpu.make_async_copy(others_b, others_b, bprecv).wait()
    total = hp[0]
    for k in range(1, PLANE):
        total = total + hp[k]
    hist_out[...] = total

    h1[0].wait_recv()
    h2 = [hop(p1, p2, 0, c3, 0, 0, 4, up)]
    h1[1].wait_recv()
    h2 += [hop(m1, m2, 0, c3, 0, 0, 5, down), hop(p1, p2, c3, c2, 0, 0, 6, up), hop(m1, m2, c3, c2, 0, 0, 7, down)]
    h1[2].wait_recv()
    send_chunk(1, p1)
    h1[3].wait_recv()
    send_chunk(7, m1)
    h2[0].wait_recv()
    h3 = [hop(p2, p3, 0, c4, 0, 0, 8, up)]
    h2[1].wait_recv()
    h3 += [hop(m2, m3, 0, c4, 0, 0, 9, down), hop(p2, p3, c4, c3, 0, 0, 10, up), hop(m2, m3, c4, c3, 0, 0, 11, down)]
    h2[2].wait_recv()
    send_chunk(2, p2)
    h2[3].wait_recv()
    send_chunk(6, m2)
    h3[0].wait_recv()
    h4 = [hop(p3, far, 0, c4, 0, 0, 12, up)]
    h3[1].wait_recv()
    h4 += [hop(m3, far, 0, c4, 0, 128, 13, down)]
    h3[2].wait_recv()
    send_chunk(3, p3)
    h3[3].wait_recv()
    send_chunk(5, m3)
    h4[0].wait_recv()
    h4[1].wait_recv()
    send_chunk(4, far)

    for copy in h1 + h2 + h3 + h4:
        copy.wait_send()
    pltpu.make_async_copy(seven, seven, hzsend).wait()
    pltpu.make_async_copy(seven_b, seven_b, bzsend).wait()
    pltpu.make_async_copy(others, others, hpsend).wait()
    pltpu.make_async_copy(others_b, others_b, bpsend).wait()
    sent = stage.at[pl.ds(0, NZ * (PLANE - 1) * 4)]
    pltpu.make_async_copy(sent, sent, psend).wait()
    pltpu.make_async_copy(stage, rows_out, precv).wait()


def exchange_rows(tier, idx, packed, bins, hist):
    caps = TIERS[tier]
    c1, c2, c3, c4 = caps
    vmem = pl.BlockSpec(memory_space=pltpu.VMEM)
    rows = lambda n: pltpu.VMEM((n, 16, 128), jnp.int32)
    dma = pltpu.SemaphoreType.DMA
    return pl.pallas_call(
        functools.partial(main_kernel, caps),
        out_shape=(
            jax.ShapeDtypeStruct((NS * 4, 16, 128), jnp.int32),
            jax.ShapeDtypeStruct((32, 128), jnp.float32),
            jax.ShapeDtypeStruct((PLANE, NZ, 4, 128), jnp.float32),
        ),
        in_specs=[pl.BlockSpec(memory_space=pltpu.SMEM), vmem, vmem, vmem],
        out_specs=(pl.BlockSpec(memory_space=pl.ANY), vmem, vmem),
        scratch_shapes=[
            rows(c1), rows(c1), rows(c2), rows(c2), rows(c3), rows(c3), rows(256),
            rows(NS * 4),
            pltpu.VMEM((NZ, 32, 128), jnp.float32), pltpu.VMEM((PLANE, 32, 128), jnp.float32),
            pltpu.VMEM((NZ, 4, 128), jnp.float32),
            dma((14,)), dma((14,)), dma, dma, dma, dma, dma, dma, dma, dma, dma, dma,
        ],
        compiler_params=pltpu.CompilerParams(
            collective_id=1 + tier, has_side_effects=True, vmem_limit_bytes=60 * 1024 * 1024),
        name=f"exchange_rows_{tier}",
    )(idx, packed, bins, hist)


def unpack_kernel(idx_ref, rows_ref, out_ref):
    block = out_ref.shape[0] // 16
    first = pl.program_id(0) * block

    def row(t, _):
        k = idx_ref[first + t]
        value = rows_ref[pl.ds(pl.multiple_of(jnp.maximum(k, 0) * 16, 16), 16), :]
        out_ref[pl.ds((t // 8) * 128 + t % 8, 16, stride=8), :] = jnp.where(k >= 0, value, 0)
        return 0

    lax.fori_loop(0, block, row, 0, unroll=8)


def unpack_rows(idx, rows):
    block = 128
    return pl.pallas_call(
        unpack_kernel,
        grid=(RECV // block,),
        out_shape=jax.ShapeDtypeStruct((RECV * 16, 128), jnp.int32),
        in_specs=[pl.BlockSpec(memory_space=pltpu.SMEM), pl.BlockSpec(memory_space=pltpu.VMEM)],
        out_specs=pl.BlockSpec((block * 16, 128), lambda i: (i, 0)),
        name="unpack_rows",
    )(idx, rows)


def layout_of(counts, z):
    owner = jnp.arange(NO)
    delta = (owner % NZ - z[..., None]) % NZ
    yo = owner // NZ
    order = jnp.where(delta <= 4, 4 - delta, delta - 4)
    side = jnp.where(delta == 4, 2, jnp.where(delta == 0, 3, jnp.where(delta < 4, 0, 1)))
    place = order * NY + yo
    before = (place[..., None, :] < place[..., :, None]) & (side[..., None, :] == side[..., :, None])
    inside = jnp.sum(jnp.where(before, counts[..., None, :], 0), axis=-1)
    flow = lambda d: jnp.sum(jnp.where(delta == d, counts, 0), axis=-1)
    f = [flow(d) for d in range(NZ)]
    plus, minus = f[1] + f[2] + f[3], f[5] + f[6] + f[7]
    split = jnp.clip((f[4] + minus - plus) // 2, 0, f[4])
    rest = f[4] - split
    first = inside + jnp.where(side == 0, split[..., None], jnp.where(side == 1, rest[..., None], 0))
    hops = [
        jnp.maximum(plus + split, minus + rest),
        jnp.maximum(f[2] + f[3] + split, f[5] + f[6] + rest),
        jnp.maximum(f[3] + split, f[5] + rest),
        jnp.maximum(split, rest),
    ]
    return first, side, split, hops


def body(keys, cut, owner, tokens):
    y, z, x, c = me()
    group = x * NC + c
    mine = y * NZ + z
    owners = jnp.arange(NO, dtype=jnp.int32)

    bins_of = keys // BIN_WIDTH
    kept = bins_of >= cut[0]
    dest = jnp.where(kept, owner[:, 0], NO)
    e = jnp.arange(EX)
    same = (dest[:, None] == dest[None, :]) & (e[None, :] < e[:, None])
    local_rank = jnp.sum(same.astype(jnp.int32), axis=1)
    onehot = dest[:, None] == owners[None, :]
    counts = jnp.sum(onehot.astype(jnp.int32), axis=0)
    row = jnp.zeros((1, 1, 128), jnp.int32).at[0, 0, :NO].set(counts)
    table = exchange_counts(row)

    first, side, split, _ = layout_of(counts, z)
    pick = lambda v: jnp.sum(jnp.where(onehot, v[None, :], 0), axis=1)
    at, on = pick(first) + local_rank, pick(side)
    far_at = jnp.where(at < split, PLUS + at, MINUS + at - split)
    pos = jnp.where(on == 0, PLUS + at, jnp.where(on == 1, MINUS + at, jnp.where(on == 2, far_at, OWN + at)))
    pos = jnp.where(kept, pos, -1).astype(jnp.int32)
    tiles = tokens.reshape(EX // 8, 8, 16, 128).transpose(0, 2, 1, 3).reshape(EX * 16, 128)
    packed = pack_rows(pos, tiles)

    tri = owners[:, None] < owners[None, :]
    sort_first = jnp.sum(jnp.where(tri, counts[:, None], 0), axis=0)
    sort_pos = jnp.where(kept, pick(sort_first) + local_rank, -1)
    bins_sorted = jnp.sum(jnp.where(sort_pos[None, :] == e[:, None], bins_of[None, :], 0), axis=1)
    bins_sorted = bins_sorted.astype(jnp.float32).reshape(4, 128)
    hi = (bins_of[:, None] // 128 == jnp.arange(32)[None, :]).astype(jnp.bfloat16)
    lo = (bins_of[:, None] % 128 == jnp.arange(128)[None, :]).astype(jnp.bfloat16)
    local_hist = lax.dot_general(hi, lo, (((0,), (0,)), ((), ())), preferred_element_type=jnp.float32)

    table = table.reshape(NY, NM, NZ, 128)[..., :NO]
    by_source = table.transpose(0, 2, 1, 3).reshape(NS, NO)
    s = jnp.arange(NS)
    lower = (s[None, :] < s[:, None]).astype(jnp.float32)
    offset = jnp.dot(lower, by_source.astype(jnp.float32), precision=lax.Precision.HIGHEST).astype(jnp.int32)

    zs_all = (s // NM) % NZ
    _, _, _, hops = layout_of(by_source, zs_all)
    tops = [jnp.max(h) for h in hops]
    tier = jnp.int32(0)
    for caps in TIERS[:-1]:
        fits = functools.reduce(jnp.logical_and, [t <= cap for t, cap in zip(tops, caps)])
        tier = tier + jnp.logical_not(fits).astype(jnp.int32)

    delta = jnp.arange(NZ)
    zs = (z - delta) % NZ
    src = (y * NZ + zs) * NM + group
    k_src, o_src = by_source[src], offset[src]
    first8, side8, split8, _ = layout_of(k_src, zs)
    rel = jnp.arange(PLANE)
    to_owner = ((y + rel // NM) % NY) * NZ + z
    to_member = ((x + (rel // NC) % NX) % NX) * NC + (c + rel % NC) % NC
    take = lambda v: v[:, to_owner][:, :, None]
    lr = (to_member[None, :, None] - take(o_src)) % NM + NM * jnp.arange(4)[None, None, :]
    q = take(first8) + lr
    far_q = jnp.where(q < split8[:, None, None], q, 128 + q - split8[:, None, None])
    q = jnp.where(take(side8) == 2, far_q, q)
    q = q + jnp.where(delta == 0, OWN, 0)[:, None, None]
    idx = jnp.where(lr < take(k_src), q, 0).astype(jnp.int32).reshape(NS * 4)

    branches = [functools.partial(exchange_rows, t) for t in range(len(TIERS))]
    rows, hist, bins_all = lax.switch(tier, branches, idx, packed.reshape(PACKED, 16, 128), bins_sorted, local_hist)
    rows = rows.reshape(NS * 64, 128)

    cnt, off = by_source[:, mine], offset[:, mine]
    lr0 = (group - off) % NM
    n = jnp.maximum(0, (cnt - lr0 + NM - 1) // NM)
    start = jnp.sum(jnp.where(s[None, :] < s[:, None], n[None, :], 0), axis=1)
    slot = jnp.arange(RECV)
    hit = (start[None, :] <= slot[:, None]) & (slot[:, None] < (start + n)[None, :])
    out_idx = jnp.sum(jnp.where(hit, 4 * s[None, :] + slot[:, None] - start[None, :] + 1, 0), axis=1) - 1
    out = unpack_rows(out_idx.astype(jnp.int32), rows)
    packed_rows = out.reshape(RECV // 8, 16, 8, 128).transpose(0, 2, 1, 3).reshape(RECV, 16 * 128)

    hist = hist.reshape(BINS)
    suffix = jnp.cumsum(hist[::-1])[::-1]
    total = jnp.maximum(suffix[cut[0]], 1.0)
    all_first = jnp.sum(jnp.where(owners[None, :] < mine, by_source, 0), axis=1)
    where_bin = jnp.sum(jnp.where(hit, (all_first + lr0)[None, :] + NM * (slot[:, None] - start[None, :]), 0), axis=1)
    bins_all = bins_all.reshape(NY, NM, NZ, EX).transpose(0, 2, 1, 3).reshape(NS, EX)
    lines = jnp.dot(hit.astype(jnp.float32), bins_all, precision=lax.Precision.HIGHEST)
    got = jnp.sum(jnp.where(where_bin[:, None] == e[None, :], lines, 0.0), axis=1)
    got = jnp.round(got).astype(jnp.int32)
    at_hi = (got[:, None] // 64 == jnp.arange(64)[None, :]).astype(jnp.float32)
    suf = jnp.dot(at_hi, suffix.reshape(64, 64), precision=lax.Precision.HIGHEST)
    suf = jnp.sum(jnp.where(got[:, None] % 64 == jnp.arange(64)[None, :], suf, 0.0), axis=1)
    packed_weights = jnp.where(out_idx >= 0, suf / total, 0.0)
    return hist.astype(jnp.int32), packed_rows, packed_weights


def solution(mesh):
    torus = Mesh(mesh.devices.reshape(NY, NZ, NX, NC), AXES)
    return jax.shard_map(
        body,
        mesh=torus,
        in_specs=(P(AXES), P(), P(AXES, None), P(AXES, None)),
        out_specs=(P(), P(AXES, None), P(AXES)),
        check_vma=False,
    )
```

```python
import functools

import jax
import jax.numpy as jnp
from jax import lax
from jax.experimental import pallas as pl
from jax.experimental.pallas import tpu as pltpu
from jax.sharding import Mesh
from jax.sharding import PartitionSpec as P

BINS = 4096
BIN_WIDTH = 262144
NY, NZ, NX, NC = 4, 8, 4, 2
NO = NY * NZ
NM = NX * NC
NS = NO * NM
PLANE = NY * NM
EX = 512
RECV = 1024
MESH_ID = pl.DeviceIdType.MESH
AXES = ("y", "z", "x", "c")

TIERS = (
    (208, 168, 120, 72),
    (232, 192, 136, 80),
    (256, 208, 152, 96),
    (384, 264, 256, 128),
)
PLUS, OWN, MINUS = 0, 384, 512
PACKED = 896


def me():
    return tuple(lax.axis_index(a) for a in AXES)


def signal_all(bar, z, y, x, c):
    def ring(d, _):
        pl.semaphore_signal(bar, 1, device_id={"z": lax.rem(z + d, NZ)}, device_id_type=MESH_ID)
        return 0

    def plane(r, _):
        pl.semaphore_signal(bar, 1, device_id=in_plane(r, y, x, c), device_id_type=MESH_ID)
        return 0

    lax.fori_loop(1, NZ, ring, 0)
    lax.fori_loop(1, PLANE, plane, 0)


def signal_peers(bar, z, y, x, c):
    signal_all(bar, z, y, x, c)
    pl.semaphore_wait(bar, NZ - 1 + PLANE - 1)


def plane_of(r, y, x, c):
    to = in_plane(r, y, x, c)
    return to["y"] * NM + to["x"] * NC + to["c"]


def in_plane(r, y, x, c):
    return {
        "y": lax.rem(y + r // NM, NY),
        "x": lax.rem(x + (r // NC) % NX, NX),
        "c": lax.rem(c + r % NC, NC),
    }

HIGHEST = lax.Precision.HIGHEST
F32, BF16, I32 = jnp.float32, jnp.bfloat16, jnp.int32


def iota(shape, dim):
    return lax.broadcasted_iota(I32, shape, dim)


def mul(a, b, contract=(1, 0), exact=False):
    dims = (((contract[0],), (contract[1],)), ((), ()))
    if exact:
        return lax.dot_general(a.astype(F32), b.astype(F32), dims, precision=HIGHEST, preferred_element_type=F32)
    return lax.dot_general(a.astype(BF16), b.astype(BF16), dims, preferred_element_type=F32)


def tmul(a, b, exact=False):
    return mul(a, b, (0, 0), exact)


def f32(mask):
    return jnp.where(mask, 1.0, 0.0).astype(F32)


def source_of(t):
    p, z = t >> 3, t & 7
    return ((p >> 3) * NZ + z) * NM + (p & 7)


L_FIRST, L_SPLIT, L_HOP, L_BIN = 32, 64, 65, 96


def stats_kernel(cut_ref, keys_ref, owner_ref, tok_hbm,
                 table_ref, idx_ref, src_ref, tier_ref, bins_ref, hist_ref, rows_ref,
                 tok_ref, row_ref, ring_ref, tok_sem, send1, send2, recv1, recv2):
    y, z, x, c = me()
    load = pltpu.make_async_copy(tok_hbm, tok_ref, tok_sem)
    load.start()
    bar = pltpu.get_barrier_semaphore()
    signal_all(bar, z, y, x, c)

    bins = lax.shift_right_logical(keys_ref[...], 18)
    dest = jnp.where(bins >= cut_ref[0], owner_ref[...], NO)
    hot = f32(iota((NO, EX), 0) == dest)
    before = mul(hot, f32(iota((EX, EX), 0) < iota((EX, EX), 1)))
    ones = jnp.ones((NO, 128), F32)
    count = mul(hot, jnp.ones((EX, 128), F32)).astype(I32)

    def place(o):
        delta = ((o & 7) - z) & 7
        side = jnp.where(delta == 4, 2, jnp.where(delta == 0, 3, jnp.where(delta < 4, 0, 1)))
        return delta, side, jnp.where(delta <= 4, 4 - delta, delta - 4) * NY + (o >> 3)

    d_row, s_row, p_row = place(iota((NO, NO), 0))
    d_col, s_col, p_col = place(iota((NO, NO), 1))
    inside = mul(f32((s_row == s_col) & (p_col < p_row)), count).astype(I32)
    bin_first = mul(f32((d_row == d_col) & (iota((NO, NO), 1) < iota((NO, NO), 0))), count).astype(I32)
    delta, side, _ = place(iota((NO, 128), 0))
    flow = lambda lo, hi: jnp.sum(jnp.where((delta >= lo) & (delta <= hi), count, 0), axis=0, keepdims=True)
    plus, minus, f4 = flow(1, 3), flow(5, 7), flow(4, 4)
    split = jnp.clip((f4 + minus - plus) >> 1, 0, f4)
    rest = f4 - split
    first = inside + jnp.where(side == 0, split, jnp.where(side == 1, rest, 0))
    hops = (
        jnp.maximum(plus + split, minus + rest),
        jnp.maximum(flow(2, 3) + split, flow(5, 6) + rest),
        jnp.maximum(flow(3, 3) + split, flow(5, 5) + rest),
        jnp.maximum(split, rest),
    )
    lane, o = iota((NO, 128), 1), iota((NO, 128), 0)
    row = jnp.where(lane == o, count, 0) + jnp.where(lane == L_FIRST + o, first, 0)
    row = row + jnp.where(lane == L_BIN + o, bin_first, 0)
    row = jnp.sum(row, axis=0, keepdims=True)
    lane = iota((1, 128), 1)
    row = row + jnp.where(lane == L_SPLIT, split, 0)
    for k, hop in enumerate(hops):
        row = row + jnp.where(lane == L_HOP + k, hop, 0)
    row = row.astype(F32)
    row_ref[0] = row
    ring_ref[pl.ds(z, 1)] = row.reshape(1, 1, 128)

    pl.semaphore_wait(bar, NZ - 1 + PLANE - 1)

    def start_ring(d, _):
        pltpu.make_async_remote_copy(
            row_ref.at[0], ring_ref.at[z], send1, recv1,
            device_id={"z": lax.rem(z + d, NZ)}, device_id_type=MESH_ID).start()
        return 0

    lax.fori_loop(1, NZ, start_ring, 0)

    rank = tmul(hot * before, ones).astype(I32)
    base = first + jnp.where(side == 1, MINUS, jnp.where(side == 3, OWN, 0))
    at = tmul(hot, base, exact=True).astype(I32) + rank
    far = tmul(hot, f32(side == 2)) > 0.5
    kept = tmul(hot, ones) > 0.5
    at = jnp.where(far & (at >= split), at + MINUS - split, at)
    at = jnp.where(kept, at, -1)
    e, lane = iota((EX, 128), 0), iota((EX, 128), 1)
    for g in range(PACKED // 128):
        src_ref[pl.ds(g, 1), :] = jnp.sum(jnp.where(at == g * 128 + lane, e, 0), axis=0, keepdims=True)

    pltpu.make_async_copy(ring_ref.at[pl.ds(0, NZ - 1)], ring_ref.at[pl.ds(0, NZ - 1)], recv1).wait()
    p = y * NM + x * NC + c

    def start_plane(r, _):
        pltpu.make_async_remote_copy(
            ring_ref, table_ref.at[p], send2, recv2,
            device_id=in_plane(r, y, x, c), device_id_type=MESH_ID).start()
        return 0

    lax.fori_loop(1, PLANE, start_plane, 0)
    table_ref[pl.ds(p, 1)] = ring_ref[...].reshape(1, NZ, 1, 128)

    bin_at = tmul(hot, (o & 7) * 128 + bin_first, exact=True).astype(I32) + rank
    bin_at = jnp.where(kept, bin_at, -1)
    part = iota((8, EX), 0)
    part = jnp.where(part == 0, bins >> 6, jnp.where(part == 1, bins & 63, 0))
    weight = jnp.where(iota((8, 128), 0) == 0, 64.0, 1.0)
    bin_col = tmul(part, weight)
    for k in range(NZ):
        bins_ref[k] = jnp.sum(jnp.where(bin_at == k * 128 + lane, bin_col, 0.0), axis=0, keepdims=True)
    hist = mul(f32(iota((32, EX), 0) == bins >> 7), f32(iota((128, EX), 0) == bins & 127), (1, 1))
    hist_ref[...] = hist.reshape(32, 1, 128)

    load.wait()

    def relay(i, _):
        rows_ref[i] = tok_ref[pl.ds((i // 8) * 128 + i % 8, 16, stride=8), :]
        return 0

    lax.fori_loop(0, EX, relay, 0, unroll=8)

    others = table_ref.at[pl.ds(0, PLANE - 1)]
    pltpu.make_async_copy(others, others, recv2).wait()
    every = table_ref[...].reshape(NS, 128)

    top = jnp.max(every, axis=0, keepdims=True)
    lane = iota((1, 128), 1)
    tier = jnp.int32(0)
    for caps in TIERS[:-1]:
        cap = jnp.full((1, 128), 1e6, F32)
        for k in range(4):
            cap = jnp.where(lane == L_HOP + k, float(caps[k]), cap)
        over = jnp.where((lane >= L_HOP) & (lane < L_HOP + 4) & (top > cap), 1, 0)
        tier = tier + jnp.max(over)
    tier_ref[0] = tier

    zs, t = iota((NZ, NS), 0), iota((NZ, NS), 1)
    offset = mul(f32(source_of(t) < source_of(p * NZ + zs)), every).astype(I32) & 7
    lane, line = iota((128, 128), 1), iota((128, 128), 0)
    owner = ((y + (lane >> 5)) & 3) * NZ + z
    mine = ring_ref[...].reshape(NZ, 128)
    cnt = mul(mine, f32(line == owner)).astype(I32)
    off = mul(offset, f32(line == owner)).astype(I32)
    fst = mul(mine, f32(line == L_FIRST + owner), exact=True).astype(I32)
    spl = mul(mine, f32(line == L_SPLIT), exact=True).astype(I32)
    lane, zs = iota((NZ, 128), 1), iota((NZ, 128), 0)
    rel = lane >> 2
    member = ((x + (rel >> 1)) & 3) * NC + ((c + rel) & 1)
    lr = ((member - off) & 7) + NM * (lane & 3)
    q = fst + lr
    delta = (z - zs) & 7
    q = jnp.where((delta == 4) & (q >= spl), 128 + q - spl, q)
    q = jnp.where(delta == 0, OWN + q, q)
    idx_ref[...] = jnp.where(lr < cnt, q, 0)

    pltpu.make_async_copy(ring_ref.at[pl.ds(0, NZ - 1)], ring_ref.at[pl.ds(0, NZ - 1)], send1).wait()
    pltpu.make_async_copy(others, others, send2).wait()


def exchange_stats(cut, keys, owner, tokens):
    vmem, smem = pl.BlockSpec(memory_space=pltpu.VMEM), pl.BlockSpec(memory_space=pltpu.SMEM)
    dma = pltpu.SemaphoreType.DMA
    shape = jax.ShapeDtypeStruct
    return pl.pallas_call(
        stats_kernel,
        out_shape=(
            shape((PLANE, NZ, 1, 128), F32),
            shape((NZ, 128), I32),
            shape((PACKED // 128, 128), I32),
            shape((1,), I32),
            shape((NZ, 1, 128), F32),
            shape((32, 1, 128), F32),
            shape((EX, 16, 128), I32),
        ),
        in_specs=[smem, vmem, vmem, pl.BlockSpec(memory_space=pl.ANY)],
        out_specs=(vmem, vmem, vmem, smem, vmem, vmem, vmem),
        scratch_shapes=[
            pltpu.VMEM((EX * 16, 128), I32),
            pltpu.VMEM((1, 1, 128), F32),
            pltpu.VMEM((NZ, 1, 128), F32),
            dma, dma, dma, dma, dma,
        ],
        compiler_params=pltpu.CompilerParams(
            collective_id=0, has_side_effects=True, vmem_limit_bytes=40 * 1024 * 1024),
        name="exchange_stats",
    )(cut, keys, owner, tokens)


def main_kernel(caps, cut_ref, idx_ref, src_ref, rows_ref, table_ref, bin_ref, hist_ref,
                rows_out, hist_out, weight_out, slot_out,
                pk, p1, m1, p2, m2, p3, m3, far, stage, hrs, hrow, hz, hrow2, hall, bz, ball,
                zsend, zrecv, psend, precv, hs1, hr1, hs2, hr2, hs3, hr3, bs1, br1, bs2, br2):
    y, z, x, c = me()
    signal_peers(pltpu.get_barrier_semaphore(), z, y, x, c)
    c1, c2, c3, c4 = caps
    up, down = lax.rem(z + 1, NZ), lax.rem(z + NZ - 1, NZ)
    plane = y * NM + x * NC + c

    def remote(src, dst, send, recv, to):
        copy = pltpu.make_async_remote_copy(src, dst, send, recv, device_id=to, device_id_type=MESH_ID)
        copy.start()
        return copy

    def loop(lo, hi, step):
        def run(i, _):
            step(i)
            return 0

        lax.fori_loop(lo, hi, run, 0)

    def whole(ref, n):
        return ref.at[pl.ds(0, n)]

    def wait(ref, n, sem):
        pltpu.make_async_copy(whole(ref, n), whole(ref, n), sem).wait()

    def hop(src, dst, lo, hi, at_src, at_dst, sem, to):
        return remote(src.at[pl.ds(at_src + lo, hi - lo)], dst.at[pl.ds(at_dst + lo, hi - lo)],
                      zsend.at[sem], zrecv.at[sem], {"z": to})

    def pack(lo, hi):
        def run(i, _):
            pk[i] = rows_ref[src_ref[i >> 7, i & 127]]
            return 0

        lax.fori_loop(lo, hi, run, 0, unroll=8)

    loop(1, NZ, lambda d: remote(bin_ref.at[lax.rem(z + d, NZ)], bz.at[z], bs1, br1, {"z": lax.rem(z + d, NZ)}))
    loop(1, PLANE, lambda r: remote(hist_ref.at[plane_of(r, y, x, c)], hrs.at[plane], hs1, hr1, in_plane(r, y, x, c)))
    bz[pl.ds(z, 1)] = bin_ref[pl.ds(z, 1)]
    hrs[pl.ds(plane, 1)] = hist_ref[pl.ds(plane, 1)]

    pack(PLUS, PLUS + c2)
    h1 = [hop(pk, p1, 0, c2, PLUS, 0, 0, up)]
    pack(MINUS, MINUS + c2)
    h1 += [hop(pk, m1, 0, c2, MINUS, 0, 1, down)]
    pack(PLUS + c2, PLUS + c1)
    h1 += [hop(pk, p1, c2, c1, PLUS, 0, 2, up)]
    pack(MINUS + c2, MINUS + c1)
    h1 += [hop(pk, m1, c2, c1, MINUS, 0, 3, down)]
    pack(OWN, MINUS)

    def send_chunk(delta, src):
        zs = lax.rem(z + NZ - delta, NZ)
        base = delta * PLANE * 4

        def gather(i, _):
            stage[base + i] = src[idx_ref[zs, i]]
            return 0

        lax.fori_loop(0, PLANE * 4, gather, 0, unroll=8)
        s = ((y * NZ + zs) * NX + x) * NC + c
        loop(1, PLANE, lambda r: remote(
            stage.at[pl.ds((delta * PLANE + r) * 4, 4)], rows_out.at[pl.ds(s * 4, 4)],
            psend, precv, in_plane(r, y, x, c)))
        pltpu.make_async_copy(
            stage.at[pl.ds(delta * PLANE * 4, 4)], rows_out.at[pl.ds(s * 4, 4)], precv).start()

    wait(bz, NZ - 1, br1)
    ball[pl.ds(plane, 1)] = bz[...].reshape(1, NZ, 1, 128)
    loop(1, PLANE, lambda r: remote(bz, ball.at[plane], bs2, br2, in_plane(r, y, x, c)))
    send_chunk(0, pk)
    wait(hrs, PLANE - 1, hr1)
    line = jnp.sum(hrs[...], axis=0, keepdims=True)
    hrow[...] = line
    hz[pl.ds(z, 1)] = line
    loop(1, NZ, lambda d: remote(hrow.at[0], hz.at[z], hs2, hr2, {"z": lax.rem(z + d, NZ)}))

    h1[0].wait_recv()
    h2 = [hop(p1, p2, 0, c3, 0, 0, 4, up)]
    h1[1].wait_recv()
    h2 += [hop(m1, m2, 0, c3, 0, 0, 5, down), hop(p1, p2, c3, c2, 0, 0, 6, up), hop(m1, m2, c3, c2, 0, 0, 7, down)]
    h1[2].wait_recv()
    send_chunk(1, p1)
    h1[3].wait_recv()
    send_chunk(7, m1)

    wait(hz, NZ - 1, hr2)
    line = jnp.sum(hz[...], axis=0, keepdims=True)
    hrow2[...] = line
    hall[pl.ds(plane, 1)] = line
    loop(1, PLANE, lambda r: remote(hrow2.at[0], hall.at[plane], hs3, hr3, in_plane(r, y, x, c)))

    every = table_ref[...].reshape(NS, 128)
    mine, member = y * NZ + z, x * NC + c
    line, lane = iota((128, 128), 0), iota((128, 128), 1)
    lower = f32(source_of(iota((NS, NS), 1)) < source_of(iota((NS, NS), 0)))
    cnt = mul(every, f32(line == mine)).astype(I32)
    off = mul(lower, every).astype(I32) & 7
    off = mul(off, f32(line == mine)).astype(I32)
    bin_first = mul(every, f32(line == L_BIN + mine)).astype(I32)
    lr0 = (member - off) & 7
    n = jnp.where(cnt > lr0, (cnt - lr0 + 7) >> 3, 0)
    start = mul(lower, n).astype(I32)
    s_row, t_lane = source_of(iota((NS, 128), 0)), iota((NS, 128), 1)
    for g in range(RECV // 128):
        j = g * 128 + t_lane - start
        slot = jnp.sum(jnp.where((j >= 0) & (j < n), 4 * s_row + j + 1, 0), axis=0, keepdims=True) - 1
        slot_out[pl.ds(g, 1), :] = slot

    h2[0].wait_recv()
    h3 = [hop(p2, p3, 0, c4, 0, 0, 8, up)]
    h2[1].wait_recv()
    h3 += [hop(m2, m3, 0, c4, 0, 0, 9, down), hop(p2, p3, c4, c3, 0, 0, 10, up), hop(m2, m3, c4, c3, 0, 0, 11, down)]
    h2[2].wait_recv()
    send_chunk(2, p2)
    h2[3].wait_recv()
    send_chunk(6, m2)
    h3[0].wait_recv()
    h4 = [hop(p3, far, 0, c4, 0, 0, 12, up)]
    h3[1].wait_recv()
    h4 += [hop(m3, far, 0, c4, 0, 128, 13, down)]
    h3[2].wait_recv()
    send_chunk(3, p3)
    h3[3].wait_recv()
    send_chunk(5, m3)
    h4[0].wait_recv()
    h4[1].wait_recv()
    send_chunk(4, far)

    wait(hall, PLANE - 1, hr3)
    wait(ball, PLANE - 1, br2)
    hist = hall[...].reshape(32, 128)
    hist_out[...] = hist.astype(I32)
    tail = mul(hist, f32(line >= lane), exact=True)
    above = jnp.sum(hist, axis=1, keepdims=True) + jnp.zeros((32, 128), F32)
    above = mul(f32(iota((32, 32), 1) > iota((32, 32), 0)), above, exact=True)
    suffix = tail + above
    bin_no = iota((32, 128), 0) * 128 + iota((32, 128), 1)
    total = jnp.maximum(jnp.sum(jnp.where(bin_no == cut_ref[0], suffix, 0.0)), 1.0)
    weights = suffix / total
    bins = ball[...].reshape(NS, 128).astype(I32)
    bins_hi, bins_lo = bins >> 7, bins & 127
    ones = jnp.ones((NS, 128), F32)
    for g in range(RECV // 128):
        j = g * 128 + t_lane - start
        hit = (j >= 0) & (j < n)
        hot = f32(hit)
        spot = tmul(jnp.where(hit, bin_first + lr0 + NM * j, 0), ones).astype(I32)
        some = tmul(hot, ones) > 0.5
        hi = jnp.sum(jnp.where(spot == lane, tmul(hot, bins_hi), 0.0), axis=1, keepdims=True).astype(I32)
        lo = jnp.sum(jnp.where(spot == lane, tmul(hot, bins_lo), 0.0), axis=1, keepdims=True).astype(I32)
        got = mul(f32(iota((128, 32), 1) == hi), weights, exact=True)
        got = jnp.sum(jnp.where((lane == lo) & some, got, 0.0), axis=1, keepdims=True)
        weight_out[pl.ds(g, 1), :] = jnp.sum(jnp.where(line == lane, got, 0.0), axis=0, keepdims=True)

    for copy in h1 + h2 + h3 + h4:
        copy.wait_send()
    wait(bz, NZ - 1, bs1)
    wait(ball, PLANE - 1, bs2)
    wait(hrs, PLANE - 1, hs1)
    wait(hz, NZ - 1, hs2)
    wait(hall, PLANE - 1, hs3)
    wait(stage, NZ * (PLANE - 1) * 4, psend)
    pltpu.make_async_copy(stage, rows_out, precv).wait()


def exchange_rows(tier, cut, idx, src, rows, table, bins, hist):
    caps = TIERS[tier]
    c1, c2, c3, c4 = caps
    vmem, smem = pl.BlockSpec(memory_space=pltpu.VMEM), pl.BlockSpec(memory_space=pltpu.SMEM)
    rows_of = lambda n: pltpu.VMEM((n, 16, 128), I32)
    lines = lambda *n: pltpu.VMEM((*n, 1, 128), F32)
    dma = pltpu.SemaphoreType.DMA
    shape = jax.ShapeDtypeStruct
    return pl.pallas_call(
        functools.partial(main_kernel, caps),
        out_shape=(
            shape((NS * 4, 16, 128), I32), shape((32, 128), I32),
            shape((RECV // 128, 128), F32), shape((RECV // 128, 128), I32),
        ),
        in_specs=[smem, smem, smem, vmem, vmem, vmem, vmem],
        out_specs=(pl.BlockSpec(memory_space=pl.ANY), vmem, vmem, vmem),
        scratch_shapes=[
            rows_of(PACKED), rows_of(c1), rows_of(c1), rows_of(c2), rows_of(c2), rows_of(c3), rows_of(c3),
            rows_of(256), rows_of(NS * 4),
            lines(PLANE), lines(1), lines(NZ), lines(1), lines(PLANE), lines(NZ), lines(PLANE, NZ),
            dma((14,)), dma((14,)), *[dma] * 12,
        ],
        compiler_params=pltpu.CompilerParams(
            collective_id=1 + tier, has_side_effects=True, vmem_limit_bytes=60 * 1024 * 1024),
        name=f"exchange_rows_{tier}",
    )(cut, idx, src, rows, table, bins, hist)


def unpack_kernel(idx_ref, rows_ref, out_ref):
    block = out_ref.shape[0] // 16
    first = pl.program_id(0) * block

    def row(t, _):
        k = idx_ref[first + t]
        value = rows_ref[pl.ds(pl.multiple_of(jnp.maximum(k, 0) * 16, 16), 16), :]
        out_ref[pl.ds((t // 8) * 128 + t % 8, 16, stride=8), :] = jnp.where(k >= 0, value, 0)
        return 0

    lax.fori_loop(0, block, row, 0, unroll=8)


def unpack_rows(idx, rows):
    block = 128
    return pl.pallas_call(
        unpack_kernel,
        grid=(RECV // block,),
        out_shape=jax.ShapeDtypeStruct((RECV * 16, 128), jnp.int32),
        in_specs=[pl.BlockSpec(memory_space=pltpu.SMEM), pl.BlockSpec(memory_space=pltpu.VMEM)],
        out_specs=pl.BlockSpec((block * 16, 128), lambda i: (i, 0)),
        name="unpack_rows",
    )(idx, rows)


def body(keys, cut, owner, tokens):
    tiles = tokens.reshape(EX // 8, 8, 16, 128).transpose(0, 2, 1, 3).reshape(EX * 16, 128)
    table, idx, src, tier, bins, hist, rows = exchange_stats(
        cut, keys.reshape(1, EX), owner.reshape(1, EX), tiles)
    branches = [functools.partial(exchange_rows, t) for t in range(len(TIERS))]
    rows, hist, weights, slots = lax.switch(tier[0], branches, cut, idx, src, rows, table, bins, hist)
    out = unpack_rows(slots.reshape(RECV), rows.reshape(NS * 64, 128))
    packed_rows = out.reshape(RECV // 8, 16, 8, 128).transpose(0, 2, 1, 3).reshape(RECV, 16 * 128)
    return hist.reshape(BINS), packed_rows, weights.reshape(RECV)


def solution(mesh):
    torus = Mesh(mesh.devices.reshape(NY, NZ, NX, NC), AXES)
    return jax.shard_map(
        body,
        mesh=torus,
        in_specs=(P(AXES), P(), P(AXES, None), P(AXES, None)),
        out_specs=(P(), P(AXES, None), P(AXES)),
        check_vma=False,
    )
```

```python
import functools

import jax
import jax.numpy as jnp
from jax import lax
from jax.experimental import pallas as pl
from jax.experimental.pallas import tpu as pltpu
from jax.sharding import Mesh
from jax.sharding import PartitionSpec as P

BINS = 4096
BIN_WIDTH = 262144
NY, NZ, NX, NC = 4, 8, 4, 2
NO = NY * NZ
NM = NX * NC
NS = NO * NM
PLANE = NY * NM
EX = 512
RECV = 1024
MESH_ID = pl.DeviceIdType.MESH
AXES = ("y", "z", "x", "c")

TIERS = (
    (204, 164, 118, 70),
    (222, 180, 132, 84),
    (254, 202, 154, 94),
    (384, 264, 256, 128),
)
PLUS, OWN, MINUS = 0, 384, 512
PACKED = 896


def me():
    return tuple(lax.axis_index(a) for a in AXES)


def signal_all(bar, z, y, x, c):
    def ring(d, _):
        pl.semaphore_signal(bar, 1, device_id={"z": lax.rem(z + d, NZ)}, device_id_type=MESH_ID)
        return 0

    def plane(r, _):
        pl.semaphore_signal(bar, 1, device_id=in_plane(r, y, x, c), device_id_type=MESH_ID)
        return 0

    lax.fori_loop(1, NZ, ring, 0)
    lax.fori_loop(1, PLANE, plane, 0)


def plane_of(r, y, x, c):
    to = in_plane(r, y, x, c)
    return to["y"] * NM + to["x"] * NC + to["c"]


def in_plane(r, y, x, c):
    return {
        "y": lax.rem(y + lax.div(r, NM), NY),
        "x": lax.rem(x + lax.rem(lax.div(r, NC), NX), NX),
        "c": lax.rem(c + lax.rem(r, NC), NC),
    }

HIGHEST = lax.Precision.HIGHEST
F32, BF16, I32 = jnp.float32, jnp.bfloat16, jnp.int32


def batched(lo, hi, load, store, batch=16):
    def step(b, count):
        for k, value in enumerate([load(b, k) for k in range(count)]):
            store(b, k, value)

    def run(b, _):
        step(lo + b * batch, batch)
        return 0

    full = (hi - lo) // batch
    lax.fori_loop(0, full, run, 0)
    step(lo + full * batch, (hi - lo) % batch)


def put(ref):
    def store(b, k, value):
        ref[b + k] = value

    return store


def iota(shape, dim):
    return lax.broadcasted_iota(I32, shape, dim)


def mul(a, b, contract=(1, 0), exact=False):
    dims = (((contract[0],), (contract[1],)), ((), ()))
    if exact:
        return lax.dot_general(a.astype(F32), b.astype(F32), dims, precision=HIGHEST, preferred_element_type=F32)
    return lax.dot_general(a.astype(BF16), b.astype(BF16), dims, preferred_element_type=F32)


def tmul(a, b, exact=False):
    return mul(a, b, (0, 0), exact)


def f32(mask):
    return jnp.where(mask, 1.0, 0.0).astype(F32)


def source_of(t):
    p, z = t >> 3, t & 7
    return ((p >> 3) * NZ + z) * NM + (p & 7)


L_FIRST, L_SPLIT, L_HOP, L_BIN = 32, 64, 65, 96


def stats_kernel(cut_ref, keys_hbm, owner_hbm, tok_hbm,
                 table_ref, idx_ref, src_ref, tier_ref, bins_ref, hist_ref, rows_ref,
                 tok_ref, keys_ref, owner_ref, row_ref, ring_ref,
                 tok_sem, keys_sem, owner_sem, send1, send2, recv1, recv2):
    y, z, x, c = me()
    load_keys = pltpu.make_async_copy(keys_hbm, keys_ref, keys_sem)
    load_owner = pltpu.make_async_copy(owner_hbm, owner_ref, owner_sem)
    load = pltpu.make_async_copy(tok_hbm, tok_ref, tok_sem)
    load_keys.start()
    load_owner.start()
    load.start()
    bar = pltpu.get_barrier_semaphore()
    signal_all(bar, z, y, x, c)
    load_keys.wait()
    load_owner.wait()

    bins = lax.shift_right_logical(keys_ref[...], 18)
    dest = jnp.where(bins >= cut_ref[0], owner_ref[...], NO)
    hot = f32(iota((NO, EX), 0) == dest)
    before = mul(hot, f32(iota((EX, EX), 0) < iota((EX, EX), 1)))
    ones = jnp.ones((NO, 128), F32)
    count = mul(hot, jnp.ones((EX, 128), F32)).astype(I32)

    def place(o):
        delta = ((o & 7) - z) & 7
        side = jnp.where(delta == 4, 2, jnp.where(delta == 0, 3, jnp.where(delta < 4, 0, 1)))
        return delta, side, jnp.where(delta <= 4, 4 - delta, delta - 4) * NY + (o >> 3)

    d_row, s_row, p_row = place(iota((NO, NO), 0))
    d_col, s_col, p_col = place(iota((NO, NO), 1))
    inside = mul(f32((s_row == s_col) & (p_col < p_row)), count).astype(I32)
    bin_first = mul(f32((d_row == d_col) & (iota((NO, NO), 1) < iota((NO, NO), 0))), count).astype(I32)
    delta, side, _ = place(iota((NO, 128), 0))
    flow = lambda lo, hi: jnp.sum(jnp.where((delta >= lo) & (delta <= hi), count, 0), axis=0, keepdims=True)
    plus, minus, f4 = flow(1, 3), flow(5, 7), flow(4, 4)
    split = jnp.clip((f4 + minus - plus) >> 1, 0, f4)
    rest = f4 - split
    first = inside + jnp.where(side == 0, split, jnp.where(side == 1, rest, 0))
    hops = (
        jnp.maximum(plus + split, minus + rest),
        jnp.maximum(flow(2, 3) + split, flow(5, 6) + rest),
        jnp.maximum(flow(3, 3) + split, flow(5, 5) + rest),
        jnp.maximum(split, rest),
    )
    lane, o = iota((NO, 128), 1), iota((NO, 128), 0)
    row = jnp.where(lane == o, count, 0) + jnp.where(lane == L_FIRST + o, first, 0)
    row = row + jnp.where(lane == L_BIN + o, bin_first, 0)
    row = jnp.sum(row, axis=0, keepdims=True)
    lane = iota((1, 128), 1)
    row = row + jnp.where(lane == L_SPLIT, split, 0)
    for k, hop in enumerate(hops):
        row = row + jnp.where(lane == L_HOP + k, hop, 0)
    row = row.astype(F32)
    row_ref[0] = row
    ring_ref[pl.ds(z, 1)] = row.reshape(1, 1, 128)

    pl.semaphore_wait(bar, NZ - 1 + PLANE - 1)

    def start_ring(d, _):
        pltpu.make_async_remote_copy(
            row_ref.at[0], ring_ref.at[z], send1, recv1,
            device_id={"z": lax.rem(z + d, NZ)}, device_id_type=MESH_ID).start()
        return 0

    lax.fori_loop(1, NZ, start_ring, 0)

    rank = tmul(hot * before, ones).astype(I32)
    base = first + jnp.where(side == 1, MINUS, jnp.where(side == 3, OWN, 0))
    at = tmul(hot, base, exact=True).astype(I32) + rank
    far = tmul(hot, f32(side == 2)) > 0.5
    kept = tmul(hot, ones) > 0.5
    at = jnp.where(far & (at >= split), at + MINUS - split, at)
    at = jnp.where(kept, at, -1)
    e, lane = iota((EX, 128), 0), iota((EX, 128), 1)
    for g in range(PACKED // 128):
        src_ref[pl.ds(g, 1), :] = jnp.sum(jnp.where(at == g * 128 + lane, e, 0), axis=0, keepdims=True)

    pltpu.make_async_copy(ring_ref.at[pl.ds(0, NZ - 1)], ring_ref.at[pl.ds(0, NZ - 1)], recv1).wait()
    p = y * NM + x * NC + c

    def start_plane(r, _):
        pltpu.make_async_remote_copy(
            ring_ref, table_ref.at[p], send2, recv2,
            device_id=in_plane(r, y, x, c), device_id_type=MESH_ID).start()
        return 0

    lax.fori_loop(1, PLANE, start_plane, 0)
    table_ref[pl.ds(p, 1)] = ring_ref[...].reshape(1, NZ, 1, 128)

    bin_at = tmul(hot, (o & 7) * 128 + bin_first, exact=True).astype(I32) + rank
    bin_at = jnp.where(kept, bin_at, -1)
    part = iota((8, EX), 0)
    part = jnp.where(part == 0, bins >> 6, jnp.where(part == 1, bins & 63, 0))
    weight = jnp.where(iota((8, 128), 0) == 0, 64.0, 1.0)
    bin_col = tmul(part, weight)
    for k in range(NZ):
        bins_ref[k] = jnp.sum(jnp.where(bin_at == k * 128 + lane, bin_col, 0.0), axis=0, keepdims=True)
    hist = mul(f32(iota((32, EX), 0) == bins >> 7), f32(iota((128, EX), 0) == bins & 127), (1, 1))
    hist_ref[...] = hist.reshape(32, 1, 128)

    load.wait()

    def tiled(b, k):
        return tok_ref[pl.ds(b * 16 + (k // 8) * 128 + k % 8, 16, stride=8), :]

    batched(0, EX, tiled, put(rows_ref))

    others = table_ref.at[pl.ds(0, PLANE - 1)]
    pltpu.make_async_copy(others, others, recv2).wait()
    every = table_ref[...].reshape(NS, 128)

    top = jnp.max(every, axis=0, keepdims=True)
    lane = iota((1, 128), 1)
    tier = jnp.int32(0)
    for caps in TIERS[:-1]:
        cap = jnp.full((1, 128), 1e6, F32)
        for k in range(4):
            cap = jnp.where(lane == L_HOP + k, float(caps[k]), cap)
        over = jnp.where((lane >= L_HOP) & (lane < L_HOP + 4) & (top > cap), 1, 0)
        tier = tier + jnp.max(over)
    tier_ref[0] = tier

    zs, t = iota((NZ, NS), 0), iota((NZ, NS), 1)
    offset = mul(f32(source_of(t) < source_of(p * NZ + zs)), every).astype(I32) & 7
    lane, line = iota((128, 128), 1), iota((128, 128), 0)
    owner = ((y + (lane >> 5)) & 3) * NZ + z
    mine = ring_ref[...].reshape(NZ, 128)
    cnt = mul(mine, f32(line == owner)).astype(I32)
    off = mul(offset, f32(line == owner)).astype(I32)
    fst = mul(mine, f32(line == L_FIRST + owner), exact=True).astype(I32)
    spl = mul(mine, f32(line == L_SPLIT), exact=True).astype(I32)
    lane, zs = iota((NZ, 128), 1), iota((NZ, 128), 0)
    rel = lane >> 2
    member = ((x + (rel >> 1)) & 3) * NC + ((c + rel) & 1)
    lr = ((member - off) & 7) + NM * (lane & 3)
    q = fst + lr
    delta = (z - zs) & 7
    q = jnp.where((delta == 4) & (q >= spl), 128 + q - spl, q)
    q = jnp.where(delta == 0, OWN + q, q)
    idx_ref[...] = jnp.where(lr < cnt, q, 0)

    pltpu.make_async_copy(ring_ref.at[pl.ds(0, NZ - 1)], ring_ref.at[pl.ds(0, NZ - 1)], send1).wait()
    pltpu.make_async_copy(others, others, send2).wait()


def exchange_stats(cut, keys, owner, tokens):
    vmem, smem = pl.BlockSpec(memory_space=pltpu.VMEM), pl.BlockSpec(memory_space=pltpu.SMEM)
    hbm = pl.BlockSpec(memory_space=pltpu.HBM)
    dma = pltpu.SemaphoreType.DMA
    shape = jax.ShapeDtypeStruct
    return pl.pallas_call(
        stats_kernel,
        out_shape=(
            shape((PLANE, NZ, 1, 128), F32),
            shape((NZ, 128), I32),
            shape((PACKED // 128, 128), I32),
            shape((1,), I32),
            shape((NZ, 1, 128), F32),
            shape((32, 1, 128), F32),
            shape((EX, 16, 128), I32),
        ),
        in_specs=[smem, hbm, hbm, hbm],
        out_specs=(vmem, vmem, vmem, smem, vmem, vmem, vmem),
        scratch_shapes=[
            pltpu.VMEM((EX * 16, 128), I32),
            pltpu.VMEM((1, EX), I32),
            pltpu.VMEM((1, EX), I32),
            pltpu.VMEM((1, 1, 128), F32),
            pltpu.VMEM((NZ, 1, 128), F32),
            *[dma] * 7,
        ],
        compiler_params=pltpu.CompilerParams(
            collective_id=0, has_side_effects=True, vmem_limit_bytes=57 * 1024 * 1024),
        name="exchange_stats",
    )(cut, keys, owner, tokens)


def main_kernel(caps, cut_ref, idx_ref, src_ref, rows_ref, table_ref, bin_ref, hist_ref,
                rows_out, hist_out, weight_out, slot_out,
                pk, p1, m1, p2, m2, p3, m3, far, stage, hrs, hrow, hz, hrow2, hall, bz, ball,
                zsend, zrecv, psend, precv, hs1, hr1, hs2, hr2, hs3, hr3, bs1, br1, bs2, br2):
    y, z, x, c = me()
    bar = pltpu.get_barrier_semaphore()
    signal_all(bar, z, y, x, c)
    c1, c2, c3, c4 = caps
    up, down = lax.rem(z + 1, NZ), lax.rem(z + NZ - 1, NZ)
    plane = y * NM + x * NC + c

    def remote(src, dst, send, recv, to):
        copy = pltpu.make_async_remote_copy(src, dst, send, recv, device_id=to, device_id_type=MESH_ID)
        copy.start()
        return copy

    def loop(lo, hi, step):
        def run(i, _):
            step(i)
            return 0

        lax.fori_loop(lo, hi, run, 0)

    def whole(ref, n):
        return ref.at[pl.ds(0, n)]

    def wait(ref, n, sem):
        pltpu.make_async_copy(whole(ref, n), whole(ref, n), sem).wait()

    def hop(src, dst, lo, hi, at_src, at_dst, sem, to):
        return remote(src.at[pl.ds(at_src + lo, hi - lo)], dst.at[pl.ds(at_dst + lo, hi - lo)],
                      zsend.at[sem], zrecv.at[sem], {"z": to})

    def pack(lo, hi):
        batched(lo, hi, lambda b, k: rows_ref[src_ref[(b + k) >> 7, (b + k) & 127]], put(pk))

    pack(PLUS, PLUS + c1)
    pack(MINUS, MINUS + c1)
    pl.semaphore_wait(bar, NZ - 1 + PLANE - 1)

    loop(1, NZ, lambda d: remote(bin_ref.at[lax.rem(z + d, NZ)], bz.at[z], bs1, br1, {"z": lax.rem(z + d, NZ)}))
    h1 = [hop(pk, p1, 0, c2, PLUS, 0, 0, up), hop(pk, m1, 0, c2, MINUS, 0, 1, down),
          hop(pk, p1, c2, c1, PLUS, 0, 2, up), hop(pk, m1, c2, c1, MINUS, 0, 3, down)]
    bz[pl.ds(z, 1)] = bin_ref[pl.ds(z, 1)]
    pack(OWN, MINUS)

    def send_chunk(delta, src):
        zs = lax.rem(z + NZ - delta, NZ)
        base = delta * PLANE * 4

        batched(0, PLANE * 4, lambda b, k: src[idx_ref[zs, b + k]], lambda b, k, v: put(stage)(base + b, k, v))
        s = ((y * NZ + zs) * NX + x) * NC + c
        loop(1, PLANE, lambda r: remote(
            stage.at[pl.ds((delta * PLANE + r) * 4, 4)], rows_out.at[pl.ds(s * 4, 4)],
            psend, precv, in_plane(r, y, x, c)))
        pltpu.make_async_copy(
            stage.at[pl.ds(delta * PLANE * 4, 4)], rows_out.at[pl.ds(s * 4, 4)], precv).start()

    send_chunk(0, pk)

    loop(1, PLANE, lambda r: remote(hist_ref.at[plane_of(r, y, x, c)], hrs.at[plane], hs1, hr1, in_plane(r, y, x, c)))
    hrs[pl.ds(plane, 1)] = hist_ref[pl.ds(plane, 1)]
    wait(bz, NZ - 1, br1)
    ball[pl.ds(plane, 1)] = bz[...].reshape(1, NZ, 1, 128)
    loop(1, PLANE, lambda r: remote(bz, ball.at[plane], bs2, br2, in_plane(r, y, x, c)))
    wait(hrs, PLANE - 1, hr1)
    line = jnp.sum(hrs[...], axis=0, keepdims=True)
    hrow[...] = line
    hz[pl.ds(z, 1)] = line
    loop(1, NZ, lambda d: remote(hrow.at[0], hz.at[z], hs2, hr2, {"z": lax.rem(z + d, NZ)}))

    h1[0].wait_recv()
    h2 = [hop(p1, p2, 0, c3, 0, 0, 4, up)]
    h1[1].wait_recv()
    h2 += [hop(m1, m2, 0, c3, 0, 0, 5, down), hop(p1, p2, c3, c2, 0, 0, 6, up), hop(m1, m2, c3, c2, 0, 0, 7, down)]
    h1[2].wait_recv()
    send_chunk(1, p1)
    h1[3].wait_recv()
    send_chunk(7, m1)

    wait(hz, NZ - 1, hr2)
    line = jnp.sum(hz[...], axis=0, keepdims=True)
    hrow2[...] = line
    hall[pl.ds(plane, 1)] = line
    loop(1, PLANE, lambda r: remote(hrow2.at[0], hall.at[plane], hs3, hr3, in_plane(r, y, x, c)))

    every = table_ref[...].reshape(NS, 128)
    mine, member = y * NZ + z, x * NC + c
    line, lane = iota((128, 128), 0), iota((128, 128), 1)
    lower = f32(source_of(iota((NS, NS), 1)) < source_of(iota((NS, NS), 0)))
    cnt = mul(every, f32(line == mine)).astype(I32)
    off = mul(lower, every).astype(I32) & 7
    off = mul(off, f32(line == mine)).astype(I32)
    bin_first = mul(every, f32(line == L_BIN + mine)).astype(I32)
    lr0 = (member - off) & 7
    n = jnp.where(cnt > lr0, (cnt - lr0 + 7) >> 3, 0)
    start = mul(lower, n).astype(I32)
    s_row, t_lane = source_of(iota((NS, 128), 0)), iota((NS, 128), 1)
    for g in range(RECV // 128):
        j = g * 128 + t_lane - start
        slot = jnp.sum(jnp.where((j >= 0) & (j < n), 4 * s_row + j + 1, 0), axis=0, keepdims=True) - 1
        slot_out[pl.ds(g, 1), :] = slot

    h2[0].wait_recv()
    h3 = [hop(p2, p3, 0, c4, 0, 0, 8, up)]
    h2[1].wait_recv()
    h3 += [hop(m2, m3, 0, c4, 0, 0, 9, down), hop(p2, p3, c4, c3, 0, 0, 10, up), hop(m2, m3, c4, c3, 0, 0, 11, down)]
    h2[2].wait_recv()
    send_chunk(2, p2)
    h2[3].wait_recv()
    send_chunk(6, m2)
    h3[0].wait_recv()
    h4 = [hop(p3, far, 0, c4, 0, 0, 12, up)]
    h3[1].wait_recv()
    h4 += [hop(m3, far, 0, c4, 0, 128, 13, down)]
    h3[2].wait_recv()
    send_chunk(3, p3)
    h3[3].wait_recv()
    send_chunk(5, m3)
    h4[0].wait_recv()
    h4[1].wait_recv()
    send_chunk(4, far)

    wait(hall, PLANE - 1, hr3)
    wait(ball, PLANE - 1, br2)
    hist = hall[...].reshape(32, 128)
    hist_out[...] = hist.astype(I32)
    tail = mul(hist, f32(line >= lane), exact=True)
    above = jnp.sum(hist, axis=1, keepdims=True) + jnp.zeros((32, 128), F32)
    above = mul(f32(iota((32, 32), 1) > iota((32, 32), 0)), above, exact=True)
    suffix = tail + above
    bin_no = iota((32, 128), 0) * 128 + iota((32, 128), 1)
    total = jnp.maximum(jnp.sum(jnp.where(bin_no == cut_ref[0], suffix, 0.0)), 1.0)
    weights = suffix / total
    bins = ball[...].reshape(NS, 128).astype(I32)
    bins_hi, bins_lo = bins >> 7, bins & 127
    ones = jnp.ones((NS, 128), F32)
    for g in range(RECV // 128):
        j = g * 128 + t_lane - start
        hit = (j >= 0) & (j < n)
        hot = f32(hit)
        spot = tmul(jnp.where(hit, bin_first + lr0 + NM * j, 0), ones).astype(I32)
        some = tmul(hot, ones) > 0.5
        hi = jnp.sum(jnp.where(spot == lane, tmul(hot, bins_hi), 0.0), axis=1, keepdims=True).astype(I32)
        lo = jnp.sum(jnp.where(spot == lane, tmul(hot, bins_lo), 0.0), axis=1, keepdims=True).astype(I32)
        got = mul(f32(iota((128, 32), 1) == hi), weights, exact=True)
        got = jnp.sum(jnp.where((lane == lo) & some, got, 0.0), axis=1, keepdims=True)
        weight_out[pl.ds(g, 1), :] = jnp.sum(jnp.where(line == lane, got, 0.0), axis=0, keepdims=True)

    for copy in h1 + h2 + h3 + h4:
        copy.wait_send()
    wait(bz, NZ - 1, bs1)
    wait(ball, PLANE - 1, bs2)
    wait(hrs, PLANE - 1, hs1)
    wait(hz, NZ - 1, hs2)
    wait(hall, PLANE - 1, hs3)
    wait(stage, NZ * (PLANE - 1) * 4, psend)
    pltpu.make_async_copy(stage, rows_out, precv).wait()


def exchange_rows(tier, cut, idx, src, rows, table, bins, hist):
    caps = TIERS[tier]
    c1, c2, c3, c4 = caps
    vmem, smem = pl.BlockSpec(memory_space=pltpu.VMEM), pl.BlockSpec(memory_space=pltpu.SMEM)
    rows_of = lambda n: pltpu.VMEM((n, 16, 128), I32)
    lines = lambda *n: pltpu.VMEM((*n, 1, 128), F32)
    dma = pltpu.SemaphoreType.DMA
    shape = jax.ShapeDtypeStruct
    return pl.pallas_call(
        functools.partial(main_kernel, caps),
        out_shape=(
            shape((NS * 4, 16, 128), I32), shape((32, 128), I32),
            shape((RECV // 128, 128), F32), shape((RECV // 128, 128), I32),
        ),
        in_specs=[smem, smem, smem, vmem, vmem, vmem, vmem],
        out_specs=(pl.BlockSpec(memory_space=pl.ANY), vmem, vmem, vmem),
        scratch_shapes=[
            rows_of(PACKED), rows_of(c1), rows_of(c1), rows_of(c2), rows_of(c2), rows_of(c3), rows_of(c3),
            rows_of(256), rows_of(NS * 4),
            lines(PLANE), lines(1), lines(NZ), lines(1), lines(PLANE), lines(NZ), lines(PLANE, NZ),
            dma((14,)), dma((14,)), *[dma] * 12,
        ],
        compiler_params=pltpu.CompilerParams(
            collective_id=1 + tier, has_side_effects=True, vmem_limit_bytes=44 * 1024 * 1024),
        name=f"exchange_rows_{tier}",
    )(cut, idx, src, rows, table, bins, hist)


def unpack_kernel(slot_ref, rows_ref, hist_in, weight_in, out_ref, hist_out, weight_out):
    block = out_ref.shape[0] // 16
    first = pl.program_id(0) * block

    def load(b, k):
        row = slot_ref[first + b + k]
        return jnp.where(row >= 0, rows_ref[jnp.maximum(row, 0)], 0)

    def store(b, k, value):
        out_ref[pl.ds(b * 16 + (k // 8) * 128 + k % 8, 16, stride=8), :] = value

    batched(0, block, load, store)

    @pl.when(pl.program_id(0) == 0)
    def _():
        hist_out[...] = hist_in[...]
        weight_out[...] = weight_in[...]


def unpack_rows(slots, rows, hist, weights):
    block = 128
    vmem = pl.BlockSpec(memory_space=pltpu.VMEM)
    keep = lambda n: pl.BlockSpec((n, 128), lambda i: (0, 0))
    shape = jax.ShapeDtypeStruct
    return pl.pallas_call(
        unpack_kernel,
        grid=(RECV // block,),
        out_shape=(shape((RECV * 16, 128), I32), shape((32, 128), I32), shape((8, 128), F32)),
        in_specs=[pl.BlockSpec(memory_space=pltpu.SMEM), vmem, keep(32), keep(8)],
        out_specs=(pl.BlockSpec((block * 16, 128), lambda i: (i, 0)), keep(32), keep(8)),
        compiler_params=pltpu.CompilerParams(vmem_limit_bytes=24 * 1024 * 1024),
        name="unpack_rows",
    )(slots, rows, hist, weights)


def body(keys, cut, owner, tokens):
    tiles = tokens.reshape(EX // 8, 8, 16, 128).transpose(0, 2, 1, 3).reshape(EX * 16, 128)
    table, idx, src, tier, bins, hist, rows = exchange_stats(
        cut, keys.reshape(1, EX), owner.reshape(1, EX), tiles)
    branches = [functools.partial(exchange_rows, t) for t in range(len(TIERS))]
    rows, hist, weights, slots = lax.switch(tier[0], branches, cut, idx, src, rows, table, bins, hist)
    out, hist, weights = unpack_rows(slots.reshape(RECV), rows, hist, weights)
    packed_rows = out.reshape(RECV // 8, 16, 8, 128).transpose(0, 2, 1, 3).reshape(RECV, 16 * 128)
    return hist.reshape(BINS), packed_rows, weights.reshape(RECV)


def solution(mesh):
    torus = Mesh(mesh.devices.reshape(NY, NZ, NX, NC), AXES)
    return jax.shard_map(
        body,
        mesh=torus,
        in_specs=(P(AXES), P(), P(AXES, None), P(AXES, None)),
        out_specs=(P(), P(AXES, None), P(AXES)),
        check_vma=False,
    )
```

```python
import functools

import jax
import jax.numpy as jnp
from jax import lax
from jax.experimental import pallas as pl
from jax.experimental.pallas import tpu as pltpu
from jax.sharding import Mesh
from jax.sharding import PartitionSpec as P

BINS = 4096
BIN_WIDTH = 262144
NY, NZ, NX, NC = 4, 8, 4, 2
NO = NY * NZ
NM = NX * NC
NS = NO * NM
PLANE = NY * NM
EX = 512
RECV = 1024
MESH_ID = pl.DeviceIdType.MESH
AXES = ("y", "z", "x", "c")

TIERS = (
    (199, 161, 124, 104),
    (210, 170, 141, 84),
    (222, 179, 141, 90),
    (245, 182, 141, 117),
    (254, 200, 157, 101),
    (384, 264, 256, 128),
)
PLUS, OWN, MINUS = 0, 384, 512
PACKED = 896
HEAD = 40


def me():
    return tuple(lax.axis_index(a) for a in AXES)


def signal_all(bar, z, y, x, c):
    def ring(d, _):
        pl.semaphore_signal(bar, 1, device_id={"z": lax.rem(z + d, NZ)}, device_id_type=MESH_ID)
        return 0

    def plane(r, _):
        pl.semaphore_signal(bar, 1, device_id=in_plane(r, y, x, c), device_id_type=MESH_ID)
        return 0

    lax.fori_loop(1, NZ, ring, 0)
    lax.fori_loop(1, PLANE, plane, 0)


def plane_of(r, y, x, c):
    to = in_plane(r, y, x, c)
    return to["y"] * NM + to["x"] * NC + to["c"]


def in_plane(r, y, x, c):
    return {
        "y": lax.rem(y + lax.div(r, NM), NY),
        "x": lax.rem(x + lax.rem(lax.div(r, NC), NX), NX),
        "c": lax.rem(c + lax.rem(r, NC), NC),
    }

HIGHEST = lax.Precision.HIGHEST
F32, BF16, I32 = jnp.float32, jnp.bfloat16, jnp.int32


def batched(lo, hi, load, store, batch=16):
    def step(b, count):
        for k, value in enumerate([load(b, k) for k in range(count)]):
            store(b, k, value)

    def run(b, _):
        step(lo + b * batch, batch)
        return 0

    full = (hi - lo) // batch
    lax.fori_loop(0, full, run, 0)
    step(lo + full * batch, (hi - lo) % batch)


def put(ref):
    def store(b, k, value):
        ref[b + k] = value

    return store


def iota(shape, dim):
    return lax.broadcasted_iota(I32, shape, dim)


def mul(a, b, contract=(1, 0), exact=False):
    dims = (((contract[0],), (contract[1],)), ((), ()))
    if exact:
        return lax.dot_general(a.astype(F32), b.astype(F32), dims, precision=HIGHEST, preferred_element_type=F32)
    return lax.dot_general(a.astype(BF16), b.astype(BF16), dims, preferred_element_type=F32)


def tmul(a, b, exact=False):
    return mul(a, b, (0, 0), exact)


def f32(mask):
    return jnp.where(mask, 1.0, 0.0).astype(F32)


def source_of(t):
    p, z = t >> 3, t & 7
    return ((p >> 3) * NZ + z) * NM + (p & 7)


L_FIRST, L_SPLIT, L_HOP, L_BIN = 32, 64, 65, 96


def stats_kernel(cut_ref, keys_hbm, owner_hbm, tok_hbm,
                 table_ref, idx_ref, src_ref, tier_ref, bins_ref, hist_ref, rows_ref, up_ref, down_ref,
                 tok_ref, keys_ref, owner_ref, row_ref, ring_ref, head_up, head_down, src_smem,
                 tok_sem, keys_sem, owner_sem, src_sem, send1, send2, recv1, recv2, hsend, hrecv):
    y, z, x, c = me()
    load_keys = pltpu.make_async_copy(keys_hbm, keys_ref, keys_sem)
    load_owner = pltpu.make_async_copy(owner_hbm, owner_ref, owner_sem)
    load = pltpu.make_async_copy(tok_hbm, tok_ref, tok_sem)
    load_keys.start()
    load_owner.start()
    load.start()
    bar = pltpu.get_barrier_semaphore()
    signal_all(bar, z, y, x, c)
    load_keys.wait()
    load_owner.wait()

    bins = lax.shift_right_logical(keys_ref[...], 18)
    dest = jnp.where(bins >= cut_ref[0], owner_ref[...], NO)
    hot = f32(iota((NO, EX), 0) == dest)
    before = mul(hot, f32(iota((EX, EX), 0) < iota((EX, EX), 1)))
    ones = jnp.ones((NO, 128), F32)
    count = mul(hot, jnp.ones((EX, 128), F32)).astype(I32)

    def place(o):
        delta = ((o & 7) - z) & 7
        side = jnp.where(delta == 4, 2, jnp.where(delta == 0, 3, jnp.where(delta < 4, 0, 1)))
        return delta, side, jnp.where(delta <= 4, 4 - delta, delta - 4) * NY + (o >> 3)

    d_row, s_row, p_row = place(iota((NO, NO), 0))
    d_col, s_col, p_col = place(iota((NO, NO), 1))
    inside = mul(f32((s_row == s_col) & (p_col < p_row)), count).astype(I32)
    bin_first = mul(f32((d_row == d_col) & (iota((NO, NO), 1) < iota((NO, NO), 0))), count).astype(I32)
    delta, side, _ = place(iota((NO, 128), 0))
    flow = lambda lo, hi: jnp.sum(jnp.where((delta >= lo) & (delta <= hi), count, 0), axis=0, keepdims=True)
    plus, minus, f4 = flow(1, 3), flow(5, 7), flow(4, 4)
    split = jnp.clip((f4 + minus - plus) >> 1, 0, f4)
    rest = f4 - split
    first = inside + jnp.where(side == 0, split, jnp.where(side == 1, rest, 0))
    hops = (
        jnp.maximum(plus + split, minus + rest),
        jnp.maximum(flow(2, 3) + split, flow(5, 6) + rest),
        jnp.maximum(flow(3, 3) + split, flow(5, 5) + rest),
        jnp.maximum(split, rest),
    )
    lane, o = iota((NO, 128), 1), iota((NO, 128), 0)
    row = jnp.where(lane == o, count, 0) + jnp.where(lane == L_FIRST + o, first, 0)
    row = row + jnp.where(lane == L_BIN + o, bin_first, 0)
    row = jnp.sum(row, axis=0, keepdims=True)
    lane = iota((1, 128), 1)
    row = row + jnp.where(lane == L_SPLIT, split, 0)
    for k, hop in enumerate(hops):
        row = row + jnp.where(lane == L_HOP + k, hop, 0)
    row = row.astype(F32)
    row_ref[0] = row
    ring_ref[pl.ds(z, 1)] = row.reshape(1, 1, 128)

    pl.semaphore_wait(bar, NZ - 1 + PLANE - 1)

    def start_ring(d, _):
        pltpu.make_async_remote_copy(
            row_ref.at[0], ring_ref.at[z], send1, recv1,
            device_id={"z": lax.rem(z + d, NZ)}, device_id_type=MESH_ID).start()
        return 0

    lax.fori_loop(1, NZ, start_ring, 0)

    rank = tmul(hot * before, ones).astype(I32)
    base = first + jnp.where(side == 1, MINUS, jnp.where(side == 3, OWN, 0))
    at = tmul(hot, base, exact=True).astype(I32) + rank
    far = tmul(hot, f32(side == 2)) > 0.5
    kept = tmul(hot, ones) > 0.5
    at = jnp.where(far & (at >= split), at + MINUS - split, at)
    at = jnp.where(kept, at, -1)
    e, lane = iota((EX, 128), 0), iota((EX, 128), 1)
    for g in range(PACKED // 128):
        src_ref[pl.ds(g, 1), :] = jnp.sum(jnp.where(at == g * 128 + lane, e, 0), axis=0, keepdims=True)

    src_ref[pl.ds(7, 1), :] = jnp.zeros((1, 128), I32)
    copy = pltpu.make_async_copy(src_ref, src_smem, src_sem)
    copy.start()

    load.wait()

    def tiled(b, k):
        return tok_ref[pl.ds(b * 16 + (k // 8) * 128 + k % 8, 16, stride=8), :]

    batched(0, EX, tiled, put(rows_ref))
    copy.wait()
    heads = []
    for k, (start, buf, out, to) in enumerate((
            (PLUS, head_up, up_ref, lax.rem(z + 1, NZ)), (MINUS, head_down, down_ref, lax.rem(z + NZ - 1, NZ)))):
        batched(0, HEAD, lambda b, i, start=start: rows_ref[src_smem[start // 128, b + i]], put(buf), batch=8)
        head = pltpu.make_async_remote_copy(
            buf, out, hsend.at[k], hrecv.at[k], device_id={"z": to}, device_id_type=MESH_ID)
        head.start()
        heads.append(head)

    pltpu.make_async_copy(ring_ref.at[pl.ds(0, NZ - 1)], ring_ref.at[pl.ds(0, NZ - 1)], recv1).wait()
    p = y * NM + x * NC + c

    def start_plane(r, _):
        pltpu.make_async_remote_copy(
            ring_ref, table_ref.at[p], send2, recv2,
            device_id=in_plane(r, y, x, c), device_id_type=MESH_ID).start()
        return 0

    lax.fori_loop(1, PLANE, start_plane, 0)
    table_ref[pl.ds(p, 1)] = ring_ref[...].reshape(1, NZ, 1, 128)

    bin_at = tmul(hot, (o & 7) * 128 + bin_first, exact=True).astype(I32) + rank
    bin_at = jnp.where(kept, bin_at, -1)
    part = iota((8, EX), 0)
    part = jnp.where(part == 0, bins >> 6, jnp.where(part == 1, bins & 63, 0))
    weight = jnp.where(iota((8, 128), 0) == 0, 64.0, 1.0)
    bin_col = tmul(part, weight)
    for k in range(NZ):
        bins_ref[k] = jnp.sum(jnp.where(bin_at == k * 128 + lane, bin_col, 0.0), axis=0, keepdims=True)
    hist = mul(f32(iota((32, EX), 0) == bins >> 7), f32(iota((128, EX), 0) == bins & 127), (1, 1))
    hist_ref[...] = hist.reshape(32, 1, 128)

    others = table_ref.at[pl.ds(0, PLANE - 1)]
    pltpu.make_async_copy(others, others, recv2).wait()
    every = table_ref[...].reshape(NS, 128)

    top = jnp.max(every, axis=0, keepdims=True)
    lane = iota((1, 128), 1)
    tier = jnp.int32(len(TIERS) - 1)
    for number, caps in reversed(list(enumerate(TIERS[:-1]))):
        cap = jnp.full((1, 128), 1e6, F32)
        for k in range(4):
            cap = jnp.where(lane == L_HOP + k, float(caps[k]), cap)
        over = jnp.where((lane >= L_HOP) & (lane < L_HOP + 4) & (top > cap), 1, 0)
        tier = jnp.where(jnp.max(over) == 0, number, tier)
    tier_ref[0] = tier

    zs, t = iota((NZ, NS), 0), iota((NZ, NS), 1)
    offset = mul(f32(source_of(t) < source_of(p * NZ + zs)), every).astype(I32) & 7
    lane, line = iota((128, 128), 1), iota((128, 128), 0)
    owner = ((y + (lane >> 5)) & 3) * NZ + z
    mine = ring_ref[...].reshape(NZ, 128)
    cnt = mul(mine, f32(line == owner)).astype(I32)
    off = mul(offset, f32(line == owner)).astype(I32)
    fst = mul(mine, f32(line == L_FIRST + owner), exact=True).astype(I32)
    spl = mul(mine, f32(line == L_SPLIT), exact=True).astype(I32)
    lane, zs = iota((NZ, 128), 1), iota((NZ, 128), 0)
    rel = lane >> 2
    member = ((x + (rel >> 1)) & 3) * NC + ((c + rel) & 1)
    lr = ((member - off) & 7) + NM * (lane & 3)
    q = fst + lr
    delta = (z - zs) & 7
    q = jnp.where((delta == 4) & (q >= spl), 128 + q - spl, q)
    q = jnp.where(delta == 0, OWN + q, q)
    idx_ref[...] = jnp.where(lr < cnt, q, 0)

    pltpu.make_async_copy(ring_ref.at[pl.ds(0, NZ - 1)], ring_ref.at[pl.ds(0, NZ - 1)], send1).wait()
    pltpu.make_async_copy(others, others, send2).wait()
    for head in heads:
        head.wait()


def exchange_stats(cut, keys, owner, tokens):
    vmem, smem = pl.BlockSpec(memory_space=pltpu.VMEM), pl.BlockSpec(memory_space=pltpu.SMEM)
    hbm = pl.BlockSpec(memory_space=pltpu.HBM)
    dma = pltpu.SemaphoreType.DMA
    shape = jax.ShapeDtypeStruct
    return pl.pallas_call(
        stats_kernel,
        out_shape=(
            shape((PLANE, NZ, 1, 128), F32),
            shape((NZ, 128), I32),
            shape((PACKED // 128 + 1, 128), I32),
            shape((1,), I32),
            shape((NZ, 1, 128), F32),
            shape((32, 1, 128), F32),
            shape((EX, 16, 128), I32),
            shape((HEAD, 16, 128), I32),
            shape((HEAD, 16, 128), I32),
        ),
        in_specs=[smem, hbm, hbm, hbm],
        out_specs=(vmem, vmem, vmem, smem, vmem, vmem, vmem, vmem, vmem),
        scratch_shapes=[
            pltpu.VMEM((EX * 16, 128), I32),
            pltpu.VMEM((1, EX), I32),
            pltpu.VMEM((1, EX), I32),
            pltpu.VMEM((1, 1, 128), F32),
            pltpu.VMEM((NZ, 1, 128), F32),
            pltpu.VMEM((HEAD, 16, 128), I32),
            pltpu.VMEM((HEAD, 16, 128), I32),
            pltpu.SMEM((PACKED // 128 + 1, 128), I32),
            *[dma] * 8, dma((2,)), dma((2,)),
        ],
        compiler_params=pltpu.CompilerParams(
            collective_id=0, has_side_effects=True, vmem_limit_bytes=57 * 1024 * 1024),
        name="exchange_stats",
    )(cut, keys, owner, tokens)


def main_kernel(caps, cut_ref, idx_ref, src_ref, rows_ref, table_ref, bin_ref, hist_ref, up_ref, down_ref,
                rows_out, hist_out, weight_out, slot_out,
                pk, p1, m1, p2, m2, p3, m3, far, stage, hrs, hrow, hz, hrow2, hall, bz, ball,
                zsend, zrecv, psend, precv, hs1, hr1, hs2, hr2, hs3, hr3, bs1, br1, bs2, br2):
    y, z, x, c = me()
    bar = pltpu.get_barrier_semaphore()
    signal_all(bar, z, y, x, c)
    c1, c2, c3, c4 = caps
    up, down = lax.rem(z + 1, NZ), lax.rem(z + NZ - 1, NZ)
    plane = y * NM + x * NC + c

    def remote(src, dst, send, recv, to):
        copy = pltpu.make_async_remote_copy(src, dst, send, recv, device_id=to, device_id_type=MESH_ID)
        copy.start()
        return copy

    def loop(lo, hi, step):
        def run(i, _):
            step(i)
            return 0

        lax.fori_loop(lo, hi, run, 0)

    def whole(ref, n):
        return ref.at[pl.ds(0, n)]

    def wait(ref, n, sem):
        pltpu.make_async_copy(whole(ref, n), whole(ref, n), sem).wait()

    def hop(src, dst, lo, hi, at_src, at_dst, sem, to):
        return remote(src.at[pl.ds(at_src + lo, hi - lo)], dst.at[pl.ds(at_dst + lo, hi - lo)],
                      zsend.at[sem], zrecv.at[sem], {"z": to})

    def pack(lo, hi):
        batched(lo, hi, lambda b, k: rows_ref[src_ref[(b + k) >> 7, (b + k) & 127]], put(pk))

    pack(PLUS + HEAD, PLUS + c1)
    pack(MINUS + HEAD, MINUS + c1)
    pl.semaphore_wait(bar, NZ - 1 + PLANE - 1)

    loop(1, NZ, lambda d: remote(bin_ref.at[lax.rem(z + d, NZ)], bz.at[z], bs1, br1, {"z": lax.rem(z + d, NZ)}))
    h1 = [hop(pk, p1, HEAD, c2, PLUS, 0, 0, up), hop(pk, m1, HEAD, c2, MINUS, 0, 1, down),
          hop(pk, p1, c2, c1, PLUS, 0, 2, up), hop(pk, m1, c2, c1, MINUS, 0, 3, down)]
    bz[pl.ds(z, 1)] = bin_ref[pl.ds(z, 1)]
    batched(0, HEAD, lambda b, k: up_ref[b + k], put(p1), batch=8)
    batched(0, HEAD, lambda b, k: down_ref[b + k], put(m1), batch=8)
    pack(OWN, MINUS)

    def send_chunk(delta, src):
        zs = lax.rem(z + NZ - delta, NZ)
        base = delta * PLANE * 4

        batched(0, PLANE * 4, lambda b, k: src[idx_ref[zs, b + k]], lambda b, k, v: put(stage)(base + b, k, v))
        s = ((y * NZ + zs) * NX + x) * NC + c

        def send(i):
            r = lax.rem((c * (PLANE - i) + (1 - c) * i) * 13, PLANE)
            remote(stage.at[pl.ds((delta * PLANE + r) * 4, 4)], rows_out.at[pl.ds(s * 4, 4)],
                   psend, precv, in_plane(r, y, x, c))

        loop(1, PLANE, send)
        pltpu.make_async_copy(
            stage.at[pl.ds(delta * PLANE * 4, 4)], rows_out.at[pl.ds(s * 4, 4)], precv).start()

    send_chunk(0, pk)

    loop(1, PLANE, lambda r: remote(hist_ref.at[plane_of(r, y, x, c)], hrs.at[plane], hs1, hr1, in_plane(r, y, x, c)))
    hrs[pl.ds(plane, 1)] = hist_ref[pl.ds(plane, 1)]
    wait(bz, NZ - 1, br1)
    ball[pl.ds(plane, 1)] = bz[...].reshape(1, NZ, 1, 128)
    loop(1, PLANE, lambda r: remote(bz, ball.at[plane], bs2, br2, in_plane(r, y, x, c)))
    wait(hrs, PLANE - 1, hr1)
    line = jnp.sum(hrs[...], axis=0, keepdims=True)
    hrow[...] = line
    hz[pl.ds(z, 1)] = line
    loop(1, NZ, lambda d: remote(hrow.at[0], hz.at[z], hs2, hr2, {"z": lax.rem(z + d, NZ)}))

    h1[0].wait_recv()
    h2 = [hop(p1, p2, 0, c3, 0, 0, 4, up)]
    h1[1].wait_recv()
    h2 += [hop(m1, m2, 0, c3, 0, 0, 5, down), hop(p1, p2, c3, c2, 0, 0, 6, up), hop(m1, m2, c3, c2, 0, 0, 7, down)]
    h1[2].wait_recv()
    send_chunk(1, p1)
    h1[3].wait_recv()
    send_chunk(7, m1)

    wait(hz, NZ - 1, hr2)
    line = jnp.sum(hz[...], axis=0, keepdims=True)
    hrow2[...] = line
    hall[pl.ds(plane, 1)] = line
    loop(1, PLANE, lambda r: remote(hrow2.at[0], hall.at[plane], hs3, hr3, in_plane(r, y, x, c)))

    every = table_ref[...].reshape(NS, 128)
    mine, member = y * NZ + z, x * NC + c
    line, lane = iota((128, 128), 0), iota((128, 128), 1)
    lower = f32(source_of(iota((NS, NS), 1)) < source_of(iota((NS, NS), 0)))
    cnt = mul(every, f32(line == mine)).astype(I32)
    off = mul(lower, every).astype(I32) & 7
    off = mul(off, f32(line == mine)).astype(I32)
    bin_first = mul(every, f32(line == L_BIN + mine)).astype(I32)
    lr0 = (member - off) & 7
    n = jnp.where(cnt > lr0, (cnt - lr0 + 7) >> 3, 0)
    start = mul(lower, n).astype(I32)
    s_row, t_lane = source_of(iota((NS, 128), 0)), iota((NS, 128), 1)
    for g in range(RECV // 128):
        j = g * 128 + t_lane - start
        slot = jnp.sum(jnp.where((j >= 0) & (j < n), 4 * s_row + j + 1, 0), axis=0, keepdims=True) - 1
        slot_out[pl.ds(g, 1), :] = slot

    h2[0].wait_recv()
    h3 = [hop(p2, p3, 0, c4, 0, 0, 8, up)]
    h2[1].wait_recv()
    h3 += [hop(m2, m3, 0, c4, 0, 0, 9, down), hop(p2, p3, c4, c3, 0, 0, 10, up), hop(m2, m3, c4, c3, 0, 0, 11, down)]
    h2[2].wait_recv()
    send_chunk(2, p2)
    h2[3].wait_recv()
    send_chunk(6, m2)
    h3[0].wait_recv()
    h4 = [hop(p3, far, 0, c4, 0, 0, 12, up)]
    h3[1].wait_recv()
    h4 += [hop(m3, far, 0, c4, 0, 128, 13, down)]
    h3[2].wait_recv()
    send_chunk(3, p3)
    h3[3].wait_recv()
    send_chunk(5, m3)
    h4[0].wait_recv()
    h4[1].wait_recv()
    send_chunk(4, far)

    wait(hall, PLANE - 1, hr3)
    wait(ball, PLANE - 1, br2)
    hist = hall[...].reshape(32, 128)
    hist_out[...] = hist.astype(I32)
    tail = mul(hist, f32(line >= lane), exact=True)
    above = jnp.sum(hist, axis=1, keepdims=True) + jnp.zeros((32, 128), F32)
    above = mul(f32(iota((32, 32), 1) > iota((32, 32), 0)), above, exact=True)
    suffix = tail + above
    bin_no = iota((32, 128), 0) * 128 + iota((32, 128), 1)
    total = jnp.maximum(jnp.sum(jnp.where(bin_no == cut_ref[0], suffix, 0.0)), 1.0)
    weights = suffix / total
    bins = ball[...].reshape(NS, 128).astype(I32)
    bins_hi, bins_lo = bins >> 7, bins & 127
    ones = jnp.ones((NS, 128), F32)
    for g in range(RECV // 128):
        j = g * 128 + t_lane - start
        hit = (j >= 0) & (j < n)
        hot = f32(hit)
        spot = tmul(jnp.where(hit, bin_first + lr0 + NM * j, 0), ones).astype(I32)
        some = tmul(hot, ones) > 0.5
        hi = jnp.sum(jnp.where(spot == lane, tmul(hot, bins_hi), 0.0), axis=1, keepdims=True).astype(I32)
        lo = jnp.sum(jnp.where(spot == lane, tmul(hot, bins_lo), 0.0), axis=1, keepdims=True).astype(I32)
        got = mul(f32(iota((128, 32), 1) == hi), weights, exact=True)
        got = jnp.sum(jnp.where((lane == lo) & some, got, 0.0), axis=1, keepdims=True)
        weight_out[pl.ds(g, 1), :] = jnp.sum(jnp.where(line == lane, got, 0.0), axis=0, keepdims=True)

    for copy in h1 + h2 + h3 + h4:
        copy.wait_send()
    wait(bz, NZ - 1, bs1)
    wait(ball, PLANE - 1, bs2)
    wait(hrs, PLANE - 1, hs1)
    wait(hz, NZ - 1, hs2)
    wait(hall, PLANE - 1, hs3)
    wait(stage, NZ * (PLANE - 1) * 4, psend)
    pltpu.make_async_copy(stage, rows_out, precv).wait()


def exchange_rows(tier, cut, idx, src, rows, table, bins, hist, up, down):
    caps = TIERS[tier]
    c1, c2, c3, c4 = caps
    vmem, smem = pl.BlockSpec(memory_space=pltpu.VMEM), pl.BlockSpec(memory_space=pltpu.SMEM)
    rows_of = lambda n: pltpu.VMEM((n, 16, 128), I32)
    lines = lambda *n: pltpu.VMEM((*n, 1, 128), F32)
    dma = pltpu.SemaphoreType.DMA
    shape = jax.ShapeDtypeStruct
    return pl.pallas_call(
        functools.partial(main_kernel, caps),
        out_shape=(
            shape((NS * 4, 16, 128), I32), shape((32, 128), I32),
            shape((RECV // 128, 128), F32), shape((RECV // 128, 128), I32),
        ),
        in_specs=[smem, smem, smem, *[vmem] * 6],
        out_specs=(pl.BlockSpec(memory_space=pl.ANY), vmem, vmem, vmem),
        scratch_shapes=[
            rows_of(PACKED), rows_of(c1), rows_of(c1), rows_of(c2), rows_of(c2), rows_of(c3), rows_of(c3),
            rows_of(256), rows_of(NS * 4),
            lines(PLANE), lines(1), lines(NZ), lines(1), lines(PLANE), lines(NZ), lines(PLANE, NZ),
            dma((14,)), dma((14,)), *[dma] * 12,
        ],
        compiler_params=pltpu.CompilerParams(
            collective_id=1 + tier, has_side_effects=True, vmem_limit_bytes=44 * 1024 * 1024),
        name=f"exchange_rows_{tier}",
    )(cut, idx, src, rows, table, bins, hist, up, down)


def unpack_kernel(slot_ref, rows_ref, hist_in, weight_in, out_ref, hist_out, weight_out):
    block = out_ref.shape[0] // 16
    first = pl.program_id(0) * block

    def load(b, k):
        row = slot_ref[first + b + k]
        return jnp.where(row >= 0, rows_ref[jnp.maximum(row, 0)], 0)

    def store(b, k, value):
        out_ref[pl.ds(b * 16 + (k // 8) * 128 + k % 8, 16, stride=8), :] = value

    batched(0, block, load, store)

    @pl.when(pl.program_id(0) == 0)
    def _():
        hist_out[...] = hist_in[...]
        weight_out[...] = weight_in[...]


def unpack_rows(slots, rows, hist, weights):
    block = 128
    vmem = pl.BlockSpec(memory_space=pltpu.VMEM)
    keep = lambda n: pl.BlockSpec((n, 128), lambda i: (0, 0))
    shape = jax.ShapeDtypeStruct
    return pl.pallas_call(
        unpack_kernel,
        grid=(RECV // block,),
        out_shape=(shape((RECV * 16, 128), I32), shape((32, 128), I32), shape((8, 128), F32)),
        in_specs=[pl.BlockSpec(memory_space=pltpu.SMEM), vmem, keep(32), keep(8)],
        out_specs=(pl.BlockSpec((block * 16, 128), lambda i: (i, 0)), keep(32), keep(8)),
        compiler_params=pltpu.CompilerParams(vmem_limit_bytes=24 * 1024 * 1024),
        name="unpack_rows",
    )(slots, rows, hist, weights)


def body(keys, cut, owner, tokens):
    tiles = tokens.reshape(EX // 8, 8, 16, 128).transpose(0, 2, 1, 3).reshape(EX * 16, 128)
    table, idx, src, tier, bins, hist, rows, up, down = exchange_stats(
        cut, keys.reshape(1, EX), owner.reshape(1, EX), tiles)
    branches = [functools.partial(exchange_rows, t) for t in range(len(TIERS))]
    rows, hist, weights, slots = lax.switch(tier[0], branches, cut, idx, src, rows, table, bins, hist, up, down)
    out, hist, weights = unpack_rows(slots.reshape(RECV), rows, hist, weights)
    packed_rows = out.reshape(RECV // 8, 16, 8, 128).transpose(0, 2, 1, 3).reshape(RECV, 16 * 128)
    return hist.reshape(BINS), packed_rows, weights.reshape(RECV)


def solution(mesh):
    torus = Mesh(mesh.devices.reshape(NY, NZ, NX, NC), AXES)
    return jax.shard_map(
        body,
        mesh=torus,
        in_specs=(P(AXES), P(), P(AXES, None), P(AXES, None)),
        out_specs=(P(), P(AXES, None), P(AXES)),
        check_vma=False,
    )
```

```python
import functools

import jax
import jax.numpy as jnp
from jax import lax
from jax.experimental import pallas as pl
from jax.experimental.pallas import tpu as pltpu
from jax.sharding import Mesh
from jax.sharding import PartitionSpec as P

BINS = 4096
BIN_WIDTH = 262144
NY, NZ, NX, NC = 4, 8, 4, 2
NO = NY * NZ
NM = NX * NC
NS = NO * NM
PLANE = NY * NM
EX = 512
RECV = 1024
MESH_ID = pl.DeviceIdType.MESH
AXES = ("y", "z", "x", "c")

TIERS = (
    (199, 161, 124, 104),
    (210, 170, 141, 84),
    (222, 179, 141, 90),
    (245, 182, 141, 117),
    (254, 200, 157, 101),
    (384, 264, 256, 128),
)
PLUS, OWN, MINUS = 0, 384, 512
PACKED = 896
BLOCK = 64
HEAD = 40


def me():
    return tuple(lax.axis_index(a) for a in AXES)


def signal_all(bar, z, y, x, c):
    def ring(d, _):
        pl.semaphore_signal(bar, 1, device_id={"z": lax.rem(z + d, NZ)}, device_id_type=MESH_ID)
        return 0

    def plane(r, _):
        pl.semaphore_signal(bar, 1, device_id=in_plane(r, y, x, c), device_id_type=MESH_ID)
        return 0

    lax.fori_loop(1, NZ, ring, 0)
    lax.fori_loop(1, PLANE, plane, 0)


def plane_of(r, y, x, c):
    to = in_plane(r, y, x, c)
    return to["y"] * NM + to["x"] * NC + to["c"]


def in_plane(r, y, x, c):
    return {
        "y": lax.rem(y + lax.div(r, NM), NY),
        "x": lax.rem(x + lax.rem(lax.div(r, NC), NX), NX),
        "c": lax.rem(c + lax.rem(r, NC), NC),
    }

HIGHEST = lax.Precision.HIGHEST
F32, BF16, I32 = jnp.float32, jnp.bfloat16, jnp.int32


def batched(lo, hi, load, store, batch=16):
    def step(b, count):
        for k, value in enumerate([load(b, k) for k in range(count)]):
            store(b, k, value)

    def run(b, _):
        step(lo + b * batch, batch)
        return 0

    full = (hi - lo) // batch
    lax.fori_loop(0, full, run, 0)
    step(lo + full * batch, (hi - lo) % batch)


def put(ref):
    def store(b, k, value):
        ref[b + k] = value

    return store


def iota(shape, dim):
    return lax.broadcasted_iota(I32, shape, dim)


def mul(a, b, contract=(1, 0), exact=False):
    dims = (((contract[0],), (contract[1],)), ((), ()))
    if exact:
        return lax.dot_general(a.astype(F32), b.astype(F32), dims, precision=HIGHEST, preferred_element_type=F32)
    return lax.dot_general(a.astype(BF16), b.astype(BF16), dims, preferred_element_type=F32)


def tmul(a, b, exact=False):
    return mul(a, b, (0, 0), exact)


def f32(mask):
    return jnp.where(mask, 1.0, 0.0).astype(F32)


def source_of(t):
    p, z = t >> 3, t & 7
    return ((p >> 3) * NZ + z) * NM + (p & 7)


L_FIRST, L_SPLIT, L_HOP, L_BIN = 32, 64, 65, 96


def stats_kernel(cut_ref, keys_hbm, owner_hbm, tok_hbm,
                 table_ref, idx_ref, src_ref, tier_ref, bins_ref, hist_ref, rows_ref, up_ref, down_ref,
                 tok_ref, keys_ref, owner_ref, row_ref, ring_ref, head_up, head_down, src_smem,
                 tok_sem, keys_sem, owner_sem, src_sem, send1, send2, recv1, recv2, hsend, hrecv):
    y, z, x, c = me()
    load_keys = pltpu.make_async_copy(keys_hbm, keys_ref, keys_sem)
    load_owner = pltpu.make_async_copy(owner_hbm, owner_ref, owner_sem)
    load = pltpu.make_async_copy(tok_hbm, tok_ref, tok_sem)
    load_keys.start()
    load_owner.start()
    load.start()
    bar = pltpu.get_barrier_semaphore()
    signal_all(bar, z, y, x, c)
    load_keys.wait()
    load_owner.wait()

    bins = lax.shift_right_logical(keys_ref[...], 18)
    dest = jnp.where(bins >= cut_ref[0], owner_ref[...], NO)
    hot = f32(iota((NO, EX), 0) == dest)
    before = mul(hot, f32(iota((EX, EX), 0) < iota((EX, EX), 1)))
    ones = jnp.ones((NO, 128), F32)
    count = mul(hot, jnp.ones((EX, 128), F32)).astype(I32)

    def place(o):
        delta = ((o & 7) - z) & 7
        side = jnp.where(delta == 4, 2, jnp.where(delta == 0, 3, jnp.where(delta < 4, 0, 1)))
        return delta, side, jnp.where(delta <= 4, 4 - delta, delta - 4) * NY + (o >> 3)

    d_row, s_row, p_row = place(iota((NO, NO), 0))
    d_col, s_col, p_col = place(iota((NO, NO), 1))
    inside = mul(f32((s_row == s_col) & (p_col < p_row)), count).astype(I32)
    bin_first = mul(f32((d_row == d_col) & (iota((NO, NO), 1) < iota((NO, NO), 0))), count).astype(I32)
    delta, side, _ = place(iota((NO, 128), 0))
    flow = lambda lo, hi: jnp.sum(jnp.where((delta >= lo) & (delta <= hi), count, 0), axis=0, keepdims=True)
    plus, minus, f4 = flow(1, 3), flow(5, 7), flow(4, 4)
    split = jnp.clip((f4 + minus - plus) >> 1, 0, f4)
    rest = f4 - split
    first = inside + jnp.where(side == 0, split, jnp.where(side == 1, rest, 0))
    hops = (
        jnp.maximum(plus + split, minus + rest),
        jnp.maximum(flow(2, 3) + split, flow(5, 6) + rest),
        jnp.maximum(flow(3, 3) + split, flow(5, 5) + rest),
        jnp.maximum(split, rest),
    )
    lane, o = iota((NO, 128), 1), iota((NO, 128), 0)
    row = jnp.where(lane == o, count, 0) + jnp.where(lane == L_FIRST + o, first, 0)
    row = row + jnp.where(lane == L_BIN + o, bin_first, 0)
    row = jnp.sum(row, axis=0, keepdims=True)
    lane = iota((1, 128), 1)
    row = row + jnp.where(lane == L_SPLIT, split, 0)
    for k, hop in enumerate(hops):
        row = row + jnp.where(lane == L_HOP + k, hop, 0)
    row = row.astype(F32)
    row_ref[0] = row
    ring_ref[pl.ds(z, 1)] = row.reshape(1, 1, 128)

    pl.semaphore_wait(bar, NZ - 1 + PLANE - 1)

    def start_ring(d, _):
        pltpu.make_async_remote_copy(
            row_ref.at[0], ring_ref.at[z], send1, recv1,
            device_id={"z": lax.rem(z + d, NZ)}, device_id_type=MESH_ID).start()
        return 0

    lax.fori_loop(1, NZ, start_ring, 0)

    rank = tmul(hot * before, ones).astype(I32)
    base = first + jnp.where(side == 1, MINUS, jnp.where(side == 3, OWN, 0))
    at = tmul(hot, base, exact=True).astype(I32) + rank
    far = tmul(hot, f32(side == 2)) > 0.5
    kept = tmul(hot, ones) > 0.5
    at = jnp.where(far & (at >= split), at + MINUS - split, at)
    at = jnp.where(kept, at, -1)
    e, lane = iota((EX, 128), 0), iota((EX, 128), 1)
    for g in range(PACKED // 128):
        src_ref[pl.ds(g, 1), :] = jnp.sum(jnp.where(at == g * 128 + lane, e, 0), axis=0, keepdims=True)

    src_ref[pl.ds(7, 1), :] = jnp.zeros((1, 128), I32)
    copy = pltpu.make_async_copy(src_ref, src_smem, src_sem)
    copy.start()

    load.wait()

    def tiled(b, k):
        return tok_ref[pl.ds(b * 16 + (k // 8) * 128 + k % 8, 16, stride=8), :]

    batched(0, EX, tiled, put(rows_ref))
    copy.wait()
    heads = []
    for k, (start, buf, out, to) in enumerate((
            (PLUS, head_up, up_ref, lax.rem(z + 1, NZ)), (MINUS, head_down, down_ref, lax.rem(z + NZ - 1, NZ)))):
        batched(0, HEAD, lambda b, i, start=start: rows_ref[src_smem[start // 128, b + i]], put(buf), batch=8)
        head = pltpu.make_async_remote_copy(
            buf, out, hsend.at[k], hrecv.at[k], device_id={"z": to}, device_id_type=MESH_ID)
        head.start()
        heads.append(head)

    pltpu.make_async_copy(ring_ref.at[pl.ds(0, NZ - 1)], ring_ref.at[pl.ds(0, NZ - 1)], recv1).wait()
    p = y * NM + x * NC + c

    def start_plane(r, _):
        pltpu.make_async_remote_copy(
            ring_ref, table_ref.at[p], send2, recv2,
            device_id=in_plane(r, y, x, c), device_id_type=MESH_ID).start()
        return 0

    lax.fori_loop(1, PLANE, start_plane, 0)
    table_ref[pl.ds(p, 1)] = ring_ref[...].reshape(1, NZ, 1, 128)

    bin_at = tmul(hot, (o & 7) * 128 + bin_first, exact=True).astype(I32) + rank
    bin_at = jnp.where(kept, bin_at, -1)
    part = iota((8, EX), 0)
    part = jnp.where(part == 0, bins >> 6, jnp.where(part == 1, bins & 63, 0))
    weight = jnp.where(iota((8, 128), 0) == 0, 64.0, 1.0)
    bin_col = tmul(part, weight)
    for k in range(NZ):
        bins_ref[k] = jnp.sum(jnp.where(bin_at == k * 128 + lane, bin_col, 0.0), axis=0, keepdims=True)
    hist = mul(f32(iota((32, EX), 0) == bins >> 7), f32(iota((128, EX), 0) == bins & 127), (1, 1))
    hist_ref[...] = hist.reshape(32, 1, 128)

    others = table_ref.at[pl.ds(0, PLANE - 1)]
    pltpu.make_async_copy(others, others, recv2).wait()
    every = table_ref[...].reshape(NS, 128)

    top = jnp.max(every, axis=0, keepdims=True)
    lane = iota((1, 128), 1)
    tier = jnp.int32(len(TIERS) - 1)
    for number, caps in reversed(list(enumerate(TIERS[:-1]))):
        cap = jnp.full((1, 128), 1e6, F32)
        for k in range(4):
            cap = jnp.where(lane == L_HOP + k, float(caps[k]), cap)
        over = jnp.where((lane >= L_HOP) & (lane < L_HOP + 4) & (top > cap), 1, 0)
        tier = jnp.where(jnp.max(over) == 0, number, tier)
    tier_ref[0] = tier

    zs, t = iota((NZ, NS), 0), iota((NZ, NS), 1)
    offset = mul(f32(source_of(t) < source_of(p * NZ + zs)), every).astype(I32) & 7
    lane, line = iota((128, 128), 1), iota((128, 128), 0)
    owner = ((y + (lane >> 5)) & 3) * NZ + z
    mine = ring_ref[...].reshape(NZ, 128)
    cnt = mul(mine, f32(line == owner)).astype(I32)
    off = mul(offset, f32(line == owner)).astype(I32)
    fst = mul(mine, f32(line == L_FIRST + owner), exact=True).astype(I32)
    spl = mul(mine, f32(line == L_SPLIT), exact=True).astype(I32)
    lane, zs = iota((NZ, 128), 1), iota((NZ, 128), 0)
    rel = lane >> 2
    member = ((x + (rel >> 1)) & 3) * NC + ((c + rel) & 1)
    lr = ((member - off) & 7) + NM * (lane & 3)
    q = fst + lr
    delta = (z - zs) & 7
    q = jnp.where((delta == 4) & (q >= spl), 128 + q - spl, q)
    q = jnp.where(delta == 0, OWN + q, q)
    idx_ref[...] = jnp.where(lr < cnt, q, 0)

    pltpu.make_async_copy(ring_ref.at[pl.ds(0, NZ - 1)], ring_ref.at[pl.ds(0, NZ - 1)], send1).wait()
    pltpu.make_async_copy(others, others, send2).wait()
    for head in heads:
        head.wait()


def exchange_stats(cut, keys, owner, tokens):
    vmem, smem = pl.BlockSpec(memory_space=pltpu.VMEM), pl.BlockSpec(memory_space=pltpu.SMEM)
    hbm = pl.BlockSpec(memory_space=pltpu.HBM)
    dma = pltpu.SemaphoreType.DMA
    shape = jax.ShapeDtypeStruct
    return pl.pallas_call(
        stats_kernel,
        out_shape=(
            shape((PLANE, NZ, 1, 128), F32),
            shape((NZ, 128), I32),
            shape((PACKED // 128 + 1, 128), I32),
            shape((1,), I32),
            shape((NZ, 1, 128), F32),
            shape((32, 1, 128), F32),
            shape((EX, 16, 128), I32),
            shape((HEAD, 16, 128), I32),
            shape((HEAD, 16, 128), I32),
        ),
        in_specs=[smem, hbm, hbm, hbm],
        out_specs=(vmem, vmem, vmem, smem, vmem, vmem, vmem, vmem, vmem),
        scratch_shapes=[
            pltpu.VMEM((EX * 16, 128), I32),
            pltpu.VMEM((1, EX), I32),
            pltpu.VMEM((1, EX), I32),
            pltpu.VMEM((1, 1, 128), F32),
            pltpu.VMEM((NZ, 1, 128), F32),
            pltpu.VMEM((HEAD, 16, 128), I32),
            pltpu.VMEM((HEAD, 16, 128), I32),
            pltpu.SMEM((PACKED // 128 + 1, 128), I32),
            *[dma] * 8, dma((2,)), dma((2,)),
        ],
        compiler_params=pltpu.CompilerParams(
            collective_id=0, has_side_effects=True, vmem_limit_bytes=57 * 1024 * 1024),
        name="exchange_stats",
    )(cut, keys, owner, tokens)


def main_kernel(caps, cut_ref, idx_ref, src_ref, rows_ref, table_ref, bin_ref, hist_ref, up_ref, down_ref,
                rows_out, hist_out, weight_out, slot_out,
                pk, p1, m1, p2, m2, p3, m3, far, stage, hrs, hrow, hz, hrow2, hall, bz, ball, zero, blank_sem,
                zsend, zrecv, psend, precv, hs1, hr1, hs2, hr2, hs3, hr3, bs1, br1, bs2, br2):
    y, z, x, c = me()
    bar = pltpu.get_barrier_semaphore()
    signal_all(bar, z, y, x, c)
    c1, c2, c3, c4 = caps
    up, down = lax.rem(z + 1, NZ), lax.rem(z + NZ - 1, NZ)
    plane = y * NM + x * NC + c

    def remote(src, dst, send, recv, to):
        copy = pltpu.make_async_remote_copy(src, dst, send, recv, device_id=to, device_id_type=MESH_ID)
        copy.start()
        return copy

    def loop(lo, hi, step):
        def run(i, _):
            step(i)
            return 0

        lax.fori_loop(lo, hi, run, 0)

    def whole(ref, n):
        return ref.at[pl.ds(0, n)]

    def wait(ref, n, sem):
        pltpu.make_async_copy(whole(ref, n), whole(ref, n), sem).wait()

    def hop(src, dst, lo, hi, at_src, at_dst, sem, to):
        return remote(src.at[pl.ds(at_src + lo, hi - lo)], dst.at[pl.ds(at_dst + lo, hi - lo)],
                      zsend.at[sem], zrecv.at[sem], {"z": to})

    def pack(lo, hi):
        batched(lo, hi, lambda b, k: rows_ref[src_ref[(b + k) >> 7, (b + k) & 127]], put(pk))

    pack(PLUS + HEAD, PLUS + c1)
    pack(MINUS + HEAD, MINUS + c1)
    pl.semaphore_wait(bar, NZ - 1 + PLANE - 1)

    loop(1, NZ, lambda d: remote(bin_ref.at[lax.rem(z + d, NZ)], bz.at[z], bs1, br1, {"z": lax.rem(z + d, NZ)}))
    h1 = [hop(pk, p1, HEAD, c2, PLUS, 0, 0, up), hop(pk, m1, HEAD, c2, MINUS, 0, 1, down),
          hop(pk, p1, c2, c1, PLUS, 0, 2, up), hop(pk, m1, c2, c1, MINUS, 0, 3, down)]
    bz[pl.ds(z, 1)] = bin_ref[pl.ds(z, 1)]
    zero[...] = jnp.zeros((1, 16, 128), I32)
    blank = pltpu.make_async_copy(zero, rows_out.at[pl.ds(NS * 4, 1)], blank_sem)
    blank.start()
    batched(0, HEAD, lambda b, k: up_ref[b + k], put(p1), batch=8)
    batched(0, HEAD, lambda b, k: down_ref[b + k], put(m1), batch=8)
    pack(OWN, MINUS)

    def send_chunk(delta, src):
        zs = lax.rem(z + NZ - delta, NZ)
        base = delta * PLANE * 4

        batched(0, PLANE * 4, lambda b, k: src[idx_ref[zs, b + k]], lambda b, k, v: put(stage)(base + b, k, v))
        s = ((y * NZ + zs) * NX + x) * NC + c

        def send(i):
            r = lax.rem((c * (PLANE - i) + (1 - c) * i) * 13, PLANE)
            remote(stage.at[pl.ds((delta * PLANE + r) * 4, 4)], rows_out.at[pl.ds(s * 4, 4)],
                   psend, precv, in_plane(r, y, x, c))

        loop(1, PLANE, send)
        pltpu.make_async_copy(
            stage.at[pl.ds(delta * PLANE * 4, 4)], rows_out.at[pl.ds(s * 4, 4)], precv).start()

    send_chunk(0, pk)

    loop(1, PLANE, lambda r: remote(hist_ref.at[plane_of(r, y, x, c)], hrs.at[plane], hs1, hr1, in_plane(r, y, x, c)))
    hrs[pl.ds(plane, 1)] = hist_ref[pl.ds(plane, 1)]
    wait(bz, NZ - 1, br1)
    ball[pl.ds(plane, 1)] = bz[...].reshape(1, NZ, 1, 128)
    loop(1, PLANE, lambda r: remote(bz, ball.at[plane], bs2, br2, in_plane(r, y, x, c)))
    wait(hrs, PLANE - 1, hr1)
    line = jnp.sum(hrs[...], axis=0, keepdims=True)
    hrow[...] = line
    hz[pl.ds(z, 1)] = line
    loop(1, NZ, lambda d: remote(hrow.at[0], hz.at[z], hs2, hr2, {"z": lax.rem(z + d, NZ)}))

    h1[0].wait_recv()
    h2 = [hop(p1, p2, 0, c3, 0, 0, 4, up)]
    h1[1].wait_recv()
    h2 += [hop(m1, m2, 0, c3, 0, 0, 5, down), hop(p1, p2, c3, c2, 0, 0, 6, up), hop(m1, m2, c3, c2, 0, 0, 7, down)]
    h1[2].wait_recv()
    send_chunk(1, p1)
    h1[3].wait_recv()
    send_chunk(7, m1)

    wait(hz, NZ - 1, hr2)
    line = jnp.sum(hz[...], axis=0, keepdims=True)
    hrow2[...] = line
    hall[pl.ds(plane, 1)] = line
    loop(1, PLANE, lambda r: remote(hrow2.at[0], hall.at[plane], hs3, hr3, in_plane(r, y, x, c)))

    every = table_ref[...].reshape(NS, 128)
    mine, member = y * NZ + z, x * NC + c
    line, lane = iota((128, 128), 0), iota((128, 128), 1)
    lower = f32(source_of(iota((NS, NS), 1)) < source_of(iota((NS, NS), 0)))
    cnt = mul(every, f32(line == mine)).astype(I32)
    off = mul(lower, every).astype(I32) & 7
    off = mul(off, f32(line == mine)).astype(I32)
    bin_first = mul(every, f32(line == L_BIN + mine)).astype(I32)
    lr0 = (member - off) & 7
    n = jnp.where(cnt > lr0, (cnt - lr0 + 7) >> 3, 0)
    start = mul(lower, n).astype(I32)
    s_row, t_lane = source_of(iota((NS, 128), 0)), iota((NS, 128), 1)
    for g in range(RECV // 128):
        j = g * 128 + t_lane - start
        slot = jnp.sum(jnp.where((j >= 0) & (j < n), 4 * s_row + j - NS * 4, 0), axis=0, keepdims=True)
        slot_out[pl.ds(g, 1), :] = NS * 4 + slot

    h2[0].wait_recv()
    h3 = [hop(p2, p3, 0, c4, 0, 0, 8, up)]
    h2[1].wait_recv()
    h3 += [hop(m2, m3, 0, c4, 0, 0, 9, down), hop(p2, p3, c4, c3, 0, 0, 10, up), hop(m2, m3, c4, c3, 0, 0, 11, down)]
    h2[2].wait_recv()
    send_chunk(2, p2)
    h2[3].wait_recv()
    send_chunk(6, m2)
    h3[0].wait_recv()
    h4 = [hop(p3, far, 0, c4, 0, 0, 12, up)]
    h3[1].wait_recv()
    h4 += [hop(m3, far, 0, c4, 0, 128, 13, down)]
    h3[2].wait_recv()
    send_chunk(3, p3)
    h3[3].wait_recv()
    send_chunk(5, m3)
    h4[0].wait_recv()
    h4[1].wait_recv()
    send_chunk(4, far)

    wait(hall, PLANE - 1, hr3)
    wait(ball, PLANE - 1, br2)
    hist = hall[...].reshape(32, 128)
    hist_out[...] = hist.astype(I32)
    tail = mul(hist, f32(line >= lane), exact=True)
    above = jnp.sum(hist, axis=1, keepdims=True) + jnp.zeros((32, 128), F32)
    above = mul(f32(iota((32, 32), 1) > iota((32, 32), 0)), above, exact=True)
    suffix = tail + above
    bin_no = iota((32, 128), 0) * 128 + iota((32, 128), 1)
    total = jnp.maximum(jnp.sum(jnp.where(bin_no == cut_ref[0], suffix, 0.0)), 1.0)
    weights = suffix / total
    bins = ball[...].reshape(NS, 128).astype(I32)
    bins_hi, bins_lo = bins >> 7, bins & 127
    ones = jnp.ones((NS, 128), F32)
    for g in range(RECV // 128):
        j = g * 128 + t_lane - start
        hit = (j >= 0) & (j < n)
        hot = f32(hit)
        spot = tmul(jnp.where(hit, bin_first + lr0 + NM * j, 0), ones).astype(I32)
        some = tmul(hot, ones) > 0.5
        hi = jnp.sum(jnp.where(spot == lane, tmul(hot, bins_hi), 0.0), axis=1, keepdims=True).astype(I32)
        lo = jnp.sum(jnp.where(spot == lane, tmul(hot, bins_lo), 0.0), axis=1, keepdims=True).astype(I32)
        got = mul(f32(iota((128, 32), 1) == hi), weights, exact=True)
        got = jnp.sum(jnp.where((lane == lo) & some, got, 0.0), axis=1, keepdims=True)
        weight_out[pl.ds(g, 1), :] = jnp.sum(jnp.where(line == lane, got, 0.0), axis=0, keepdims=True)

    for copy in h1 + h2 + h3 + h4:
        copy.wait_send()
    wait(bz, NZ - 1, bs1)
    wait(ball, PLANE - 1, bs2)
    wait(hrs, PLANE - 1, hs1)
    wait(hz, NZ - 1, hs2)
    wait(hall, PLANE - 1, hs3)
    wait(stage, NZ * (PLANE - 1) * 4, psend)
    pltpu.make_async_copy(stage, rows_out.at[pl.ds(0, NS * 4)], precv).wait()
    blank.wait()


def exchange_rows(tier, cut, idx, src, rows, table, bins, hist, up, down):
    caps = TIERS[tier]
    c1, c2, c3, c4 = caps
    vmem, smem = pl.BlockSpec(memory_space=pltpu.VMEM), pl.BlockSpec(memory_space=pltpu.SMEM)
    rows_of = lambda n: pltpu.VMEM((n, 16, 128), I32)
    lines = lambda *n: pltpu.VMEM((*n, 1, 128), F32)
    dma = pltpu.SemaphoreType.DMA
    shape = jax.ShapeDtypeStruct
    return pl.pallas_call(
        functools.partial(main_kernel, caps),
        out_shape=(
            shape((NS * 4 + 1, 16, 128), I32), shape((32, 128), I32),
            shape((RECV // 128, 128), F32), shape((RECV // 128, 128), I32),
        ),
        in_specs=[smem, smem, smem, *[vmem] * 6],
        out_specs=(pl.BlockSpec(memory_space=pl.ANY), vmem, vmem, vmem),
        scratch_shapes=[
            rows_of(PACKED), rows_of(c1), rows_of(c1), rows_of(c2), rows_of(c2), rows_of(c3), rows_of(c3),
            rows_of(256), rows_of(NS * 4),
            lines(PLANE), lines(1), lines(NZ), lines(1), lines(PLANE), lines(NZ), lines(PLANE, NZ), rows_of(1), dma,
            dma((14,)), dma((14,)), *[dma] * 12,
        ],
        compiler_params=pltpu.CompilerParams(
            collective_id=1 + tier, has_side_effects=True, vmem_limit_bytes=44 * 1024 * 1024),
        name=f"exchange_rows_{tier}",
    )(cut, idx, src, rows, table, bins, hist, up, down)


def unpack_kernel(slot_ref, rows_ref, hist_in, weight_in, out_ref, hist_out, weight_out, tiles, sems, small_sems):
    copies = [pltpu.make_async_copy(hist_in, hist_out, small_sems.at[0]),
              pltpu.make_async_copy(weight_in, weight_out, small_sems.at[1])]
    for copy in copies:
        copy.start()

    def store(b, k, value):
        tiles[pl.ds(b * 16 + (k // 8) * 128 + k % 8, 16, stride=8), :] = value

    for g in range(RECV // BLOCK):
        batched(g * BLOCK, (g + 1) * BLOCK, lambda b, k: rows_ref[slot_ref[b + k]], store)
        part = pl.ds(g * BLOCK * 16, BLOCK * 16)
        copies.append(pltpu.make_async_copy(tiles.at[part], out_ref.at[part], sems.at[g]))
        copies[-1].start()
    for copy in copies:
        copy.wait()


def unpack_rows(slots, rows, hist, weights):
    vmem, out = pl.BlockSpec(memory_space=pltpu.VMEM), pl.BlockSpec(memory_space=pl.ANY)
    shape = jax.ShapeDtypeStruct
    return pl.pallas_call(
        unpack_kernel,
        out_shape=(shape((RECV * 16, 128), I32), shape((32, 128), I32), shape((8, 128), F32)),
        in_specs=[pl.BlockSpec(memory_space=pltpu.SMEM), vmem, vmem, vmem],
        out_specs=(out, out, out),
        scratch_shapes=[
            pltpu.VMEM((RECV * 16, 128), I32),
            pltpu.SemaphoreType.DMA((RECV // BLOCK,)),
            pltpu.SemaphoreType.DMA((2,)),
        ],
        compiler_params=pltpu.CompilerParams(vmem_limit_bytes=24 * 1024 * 1024),
        name="unpack_rows",
    )(slots, rows, hist, weights)


def body(keys, cut, owner, tokens):
    tiles = tokens.reshape(EX // 8, 8, 16, 128).transpose(0, 2, 1, 3).reshape(EX * 16, 128)
    table, idx, src, tier, bins, hist, rows, up, down = exchange_stats(
        cut, keys.reshape(1, EX), owner.reshape(1, EX), tiles)
    branches = [functools.partial(exchange_rows, t) for t in range(len(TIERS))]
    rows, hist, weights, slots = lax.switch(tier[0], branches, cut, idx, src, rows, table, bins, hist, up, down)
    out, hist, weights = unpack_rows(slots.reshape(RECV), rows, hist, weights)
    packed_rows = out.reshape(RECV // 8, 16, 8, 128).transpose(0, 2, 1, 3).reshape(RECV, 16 * 128)
    return hist.reshape(BINS), packed_rows, weights.reshape(RECV)


def solution(mesh):
    torus = Mesh(mesh.devices.reshape(NY, NZ, NX, NC), AXES)
    return jax.shard_map(
        body,
        mesh=torus,
        in_specs=(P(AXES), P(), P(AXES, None), P(AXES, None)),
        out_specs=(P(), P(AXES, None), P(AXES)),
        check_vma=False,
    )
```
